32 devices in a mesh: parts: 2 (over y), replica: 4 (over x, core), tensor: 4 (over z).
Axes of the slice: x: 2, y: 2, z: 4, core: 2. Of those that a mesh axis runs over, the one named last changes fastest.
Arguments:
- prompt_owner: int32 [8], P('parts'), parts along dimension 0, may hold values from 0 to 3, each once
- fork_map: int32 [1024], P(('parts', 'replica')), parts along dimension 0, may hold values from 0 to 3
- page_table: int32 [24], P('parts'), parts along dimension 0, may hold values from 0 to 11, each once
- prompt_length: int32 [8], P('parts'), parts along dimension 0, may hold values from 1 to 384
- span_states: bfloat16 [1024, 8192], P(('parts', 'replica'), 'tensor'), parts along dimension 0, may hold values from -6 to 6
- decode_states: bfloat16 [1024, 4, 8192], P(('parts', 'replica'), None, 'tensor'), parts along dimension 0, may hold values from -6 to 6
- decode_queries: bfloat16 [1024, 4, 4096], P(('parts', 'replica'), None, 'tensor'), parts along dimension 0, may hold values from -64 to 64
- key_weight: bfloat16 [8192, 512], P('tensor'), may hold values from -0.0625 to 0.0625
- value_weight: bfloat16 [8192, 512], P('tensor'), may hold values from -0.0625 to 0.0625
- out_weight: bfloat16 [4096, 8192], P(None, 'tensor'), may hold values from -0.09375 to 0.09375
- page_pool: bfloat16 [4, 24, 128, 256], P('tensor', 'parts'), parts along dimension 1, may hold values from -6 to 60, as said below
Outputs:
- decoded: bfloat16 [1024, 4, 8192], P(('parts', 'replica'), None, 'tensor'), parts along dimension 0
The draws below stay inside these ranges and needn't reach their ends.
There are 2 independent parts, one for each index of `parts`. The reference program is written for one: setup_inputs(seed, part) draws one part's arguments, and reference() takes and returns one part's arrays. A program takes and returns all parts, laid end to end along the dimension named above; an argument that names none is the same for every part. Nothing has to cross between parts.
Inputs may be any that keep to these rules, and one draw needn't show every extreme that they name: Replica r prefills prompt prompt_owner[r]; every prompt has exactly one such replica. The cache pages of prompt p are page_table[p * 3 + c] for c below 3; every pool page belongs to exactly one prompt. page_pool[t] holds the cache of key-value head t; devices that read the same head hold equal copies.
All inputs are finite; a program needn't handle non-finite values.
Results may differ from the reference program's by a relative error of at most 0.009.
Values may be sent and summed in bfloat16 or wider, within the bound.
A program may use at most 64 MiB of HBM per device.

```python
import jax
import jax.numpy as jnp
from jax import lax

D = 8192
HD = 128
HEADS = 32
KVH = 4
SPAN = 128
STEPS = 4
PAGE = 128
CPAGES = 3
ROWS = 128
SHARE = 1
POOL = 12
ALL_ROWS = 512
ALL_SPAN = 512
N_REPLICA = 4


def draw_page_pool(key, part):
    base = jnp.clip(jax.random.normal(key, (KVH, POOL, PAGE, 2 * HD), jnp.float32), -6.0, 6.0)
    return jnp.repeat(base, SHARE, axis=0).astype(jnp.bfloat16)


def draw_decode_queries(key, part):
    base = jnp.clip(jax.random.normal(key, (ALL_ROWS, STEPS, HEADS, HD), jnp.float32), -6.0, 6.0)
    return base.reshape(ALL_ROWS, STEPS, HEADS * HD).astype(jnp.bfloat16)


def set_ends(drawn, key, smallest, high):
    index_at = [jax.random.randint(jax.random.fold_in(key, axis), (), 0, length) for axis, length in enumerate(drawn.shape)]
    main_axis = drawn.shape.index(max(drawn.shape))
    next_to = index_at[:main_axis] + [(index_at[main_axis] + 1) % drawn.shape[main_axis]] + index_at[main_axis + 1:]
    return drawn.at[tuple(index_at)].set(smallest).at[tuple(next_to)].set(high)


def steps_of(rng, extent, cuts, low, top_value):
    def one(axis_at, shards_of):
        heights = jax.random.uniform(jax.random.fold_in(jax.random.fold_in(rng, 6), axis_at), (shards_of,), jnp.float32, low / len(cuts), top_value / len(cuts))
        return jnp.repeat(jnp.exp(heights), extent[axis_at] // shards_of).reshape((-1,) + (1,) * (len(extent) - axis_at - 1))

    loudness = one(*cuts[0])
    for cut in cuts[1:]:
        loudness = loudness * one(*cut)
    return loudness


def normal_values(key, shape, spread, bound, cuts=(), kind=jnp.bfloat16):
    values = spread * jax.random.normal(key, shape, jnp.float32)
    if cuts:
        values = values * steps_of(key, shape, cuts, -0.22, 0.18)
    return jnp.clip(values, -bound, bound).astype(kind)


def setup_inputs(seed: int = 0, part: int = 0) -> dict:
    key_list = jax.random.split(jax.random.key(seed), 12)
    part_splits = jax.random.split(jax.random.fold_in(key_list[11], part), 12)
    prompt_owner = jax.random.permutation(part_splits[0], N_REPLICA).astype(jnp.int32)
    fork_map = set_ends(jax.random.randint(part_splits[1], (ALL_ROWS,), 0, N_REPLICA), jax.random.fold_in(part_splits[1], 1), 0, N_REPLICA - 1).astype(jnp.int32)
    page_table = jax.random.permutation(part_splits[2], POOL).astype(jnp.int32)
    prompt_length = set_ends(jax.random.randint(part_splits[3], (N_REPLICA,), 1, CPAGES * PAGE + 1), jax.random.fold_in(part_splits[3], 1), 1, CPAGES * PAGE).astype(jnp.int32)
    span_states = normal_values(part_splits[4], (ALL_SPAN, D), 1.0, 6.0, ((0, 4), (1, 4)))
    decode_states = normal_values(part_splits[5], (ALL_ROWS, STEPS, D), 1.0, 6.0, ((0, 4), (2, 4)))
    decode_queries = draw_decode_queries(jax.random.fold_in(jax.random.fold_in(key_list[11], part), 71), part)
    key_weight = normal_values(key_list[7], (D, KVH * HD), D ** -0.5, 0.0625, ((0, 4),))
    value_weight = normal_values(key_list[8], (D, KVH * HD), D ** -0.5, 0.0625, ((0, 4),))
    out_weight = normal_values(key_list[9], (HEADS * HD, D), (HEADS * HD) ** -0.5, 0.09375, ((1, 4),))
    page_pool = draw_page_pool(jax.random.fold_in(jax.random.fold_in(key_list[11], part), 71), part)
    return dict(prompt_owner=prompt_owner, fork_map=fork_map, page_table=page_table, prompt_length=prompt_length, span_states=span_states, decode_states=decode_states, decode_queries=decode_queries, key_weight=key_weight, value_weight=value_weight, out_weight=out_weight, page_pool=page_pool)


rope_base = 1000000.0


def rotary(vectors, places):
    half = vectors.shape[-1] // 2
    freq = rope_base ** (-(2.0 / vectors.shape[-1]) * jnp.arange(half, dtype=jnp.float32))
    angle = places.astype(jnp.float32)[..., None, None] * freq
    cosine = jnp.cos(angle)
    sine = jnp.sin(angle)
    first = vectors[..., :half]
    second = vectors[..., half:]
    return jnp.concatenate([first * cosine - second * sine, second * cosine + first * sine], -1)


def reference(prompt_owner, fork_map, page_table, prompt_length, span_states, decode_states, decode_queries, key_weight, value_weight, out_weight, page_pool):
    weights = jnp.concatenate([key_weight, value_weight], 1)
    tokens = jnp.concatenate([span_states, decode_states.reshape(ALL_ROWS * STEPS, D)], 0)
    projected = jnp.dot(tokens, weights, preferred_element_type=jnp.float32)
    span_places = prompt_length[prompt_owner][:, None] + jnp.arange(SPAN, dtype=jnp.int32)[None, :]
    tail_places = prompt_length[fork_map][:, None] + SPAN + jnp.arange(STEPS, dtype=jnp.int32)[None, :]
    positions = jnp.concatenate([span_places.reshape(-1), tail_places.reshape(-1)]).astype(jnp.int32)
    number = positions.shape[0]
    new_keys = rotary(projected[:, :KVH * HD].reshape(number, KVH, HD), positions).astype(jnp.bfloat16)
    new_values = projected[:, KVH * HD:].reshape(number, KVH, HD).astype(jnp.bfloat16)
    span_keys = new_keys[:ALL_SPAN]
    span_values = new_values[:ALL_SPAN]
    tail_keys = new_keys[ALL_SPAN:].reshape(N_REPLICA, ROWS, STEPS, KVH, HD)
    tail_values = new_values[ALL_SPAN:].reshape(N_REPLICA, ROWS, STEPS, KVH, HD)
    entries = jnp.arange(POOL, dtype=jnp.int32)
    page_prompt = jnp.zeros((POOL,), jnp.int32).at[page_table].set(entries // CPAGES)
    page_slot = jnp.zeros((POOL,), jnp.int32).at[page_table].set(entries % CPAGES)
    cached_places = page_slot[:, None] * PAGE + jnp.arange(PAGE, dtype=jnp.int32)[None, :]
    visible = cached_places < prompt_length[page_prompt][:, None]
    pool_prompt = jnp.where(visible, page_prompt[:, None], -1).reshape(-1)
    key_prompt = jnp.concatenate([pool_prompt, jnp.repeat(prompt_owner, SPAN)]).astype(jnp.int32)
    group = HEADS // KVH
    scale = HD ** -0.5
    causal = jnp.arange(STEPS)[None, :] <= jnp.arange(STEPS)[:, None]
    queries = decode_queries.reshape(N_REPLICA, ROWS, STEPS, HEADS, HD)
    row_prompts = fork_map.reshape(N_REPLICA, ROWS)

    def one_replica(items):
        query, prompt, own_keys, own_values = items
        pieces = []
        for head_group in range(KVH):
            cache = page_pool[head_group * SHARE].reshape(POOL * PAGE, 2 * HD)
            key_table = jnp.concatenate([cache[:, :HD], span_keys[:, head_group]], 0).astype(jnp.float32)
            value_table = jnp.concatenate([cache[:, HD:], span_values[:, head_group]], 0).astype(jnp.float32)
            local = query[:, :, head_group * group:(head_group + 1) * group].astype(jnp.float32)
            scores = jnp.einsum("rshd,kd->rshk", local, key_table) * scale
            allowed = (key_prompt[None, :] == prompt[:, None])[:, None, None, :]
            scores = jnp.where(allowed, scores, -jnp.inf)
            tail_key = own_keys[:, :, head_group].astype(jnp.float32)
            tail_value = own_values[:, :, head_group].astype(jnp.float32)
            tail = jnp.einsum("rshd,rtd->rsht", local, tail_key) * scale
            tail = jnp.where(causal[None, :, None, :], tail, -jnp.inf)
            highest = jnp.maximum(jnp.max(scores, -1), jnp.max(tail, -1))
            weight = jnp.exp(scores - highest[..., None])
            tail_weight = jnp.exp(tail - highest[..., None])
            total = jnp.sum(weight, -1) + jnp.sum(tail_weight, -1)
            mixed = jnp.einsum("rshk,kd->rshd", weight.astype(jnp.bfloat16).astype(jnp.float32), value_table)
            mixed = mixed + jnp.einsum("rsht,rtd->rshd", tail_weight.astype(jnp.bfloat16).astype(jnp.float32), tail_value)
            pieces.append((mixed / total[..., None]).astype(jnp.bfloat16))
        return jnp.concatenate(pieces, 2)

    attended = lax.map(one_replica, (queries, row_prompts, tail_keys, tail_values))
    flat = attended.reshape(ALL_ROWS * STEPS, HEADS * HD)
    decoded = jnp.dot(flat, out_weight, preferred_element_type=jnp.float32).astype(jnp.bfloat16)
    return decoded.reshape(ALL_ROWS, STEPS, D)
```

```python
import functools
import math

import jax
import jax.numpy as jnp
from jax import lax
from jax.experimental import pallas as pl
from jax.experimental.pallas import tpu as pltpu
from jax.sharding import PartitionSpec as P

HD = 128


rope_base = 1000000.0


def rotary(vectors, places):
    half = vectors.shape[-1] // 2
    freq = rope_base ** (-(2.0 / vectors.shape[-1]) * jnp.arange(half, dtype=jnp.float32))
    angle = places.astype(jnp.float32)[..., None, None] * freq
    cosine = jnp.cos(angle)
    sine = jnp.sin(angle)
    first = vectors[..., :half]
    second = vectors[..., half:]
    return jnp.concatenate([first * cosine - second * sine, second * cosine + first * sine], -1)


def rotate_round(summed, places, kv_heads):
    number = summed.shape[0]
    turned = rotary(summed[:, : kv_heads * HD].reshape(number, kv_heads, HD), places)
    turned = turned.astype(jnp.bfloat16).reshape(number, kv_heads * HD)
    return jnp.concatenate([turned, summed[:, kv_heads * HD :].astype(jnp.bfloat16)], 1)


def own_pair(packed, head_group, kv_heads):
    key_part = lax.dynamic_slice_in_dim(packed, head_group * HD, HD, 1)
    value_part = lax.dynamic_slice_in_dim(packed, (kv_heads + head_group) * HD, HD, 1)
    return jnp.concatenate([key_part, value_part], 1)


def general(
    prompt_owner,
    fork_map,
    page_table,
    prompt_length,
    span_states,
    decode_states,
    decode_queries,
    key_weight,
    value_weight,
    out_weight,
    page_pool,
):
    replica = lax.axis_index("replica")
    device_rank = lax.axis_index("tensor")
    n_replica = lax.axis_size("replica")
    n_tensor = lax.axis_size("tensor")
    span = span_states.shape[0]
    rows, steps, width = decode_states.shape
    heads_dev = decode_queries.shape[2] // HD
    kv_heads = key_weight.shape[1] // HD
    sharing = n_tensor // kv_heads
    prompts = jnp.arange(n_replica, dtype=jnp.int32)
    own_prompt = jnp.sum(jnp.where(prompts == replica, prompt_owner, 0))
    own_length = jnp.sum(jnp.where(prompts == own_prompt, prompt_length, 0))
    row_hits = fork_map[:, None] == prompts[None, :]
    row_length = jnp.sum(jnp.where(row_hits, prompt_length[None, :], 0), 1)
    positions = jnp.concatenate(
        [
            own_length + jnp.arange(span, dtype=jnp.int32),
            (row_length[:, None] + span + jnp.arange(steps, dtype=jnp.int32)[None, :]).reshape(-1),
        ]
    )
    tokens = jnp.concatenate([span_states, decode_states.reshape(rows * steps, width)], 0)
    projected = jnp.dot(
        tokens, jnp.concatenate([key_weight, value_weight], 1), preferred_element_type=jnp.float32
    )
    share = lax.psum_scatter(projected, "tensor", scatter_dimension=0, tiled=True)
    number = share.shape[0]
    start = device_rank * number
    places = lax.dynamic_slice_in_dim(positions, start, number)
    turned = rotate_round(share, places, kv_heads)
    groups = jnp.stack(
        [own_pair(turned, group_index, kv_heads) for group_index in range(kv_heads)], 0
    )
    outgoing = jnp.repeat(groups, sharing, axis=0)
    paired = lax.all_to_all(outgoing, "tensor", split_axis=0, concat_axis=1, tiled=True).reshape(
        -1, 2 * HD
    )
    arrived = lax.all_gather(paired[:span], "replica", axis=0, tiled=True)
    tail_pair = paired[span:].reshape(rows, steps, 2 * HD)
    pool_pages = page_table.shape[0]
    cpages = pool_pages // n_replica
    page_size = page_pool.shape[2]
    entries = jnp.arange(pool_pages, dtype=jnp.int32)
    page_hits = page_table[None, :] == entries[:, None]
    page_prompt = jnp.sum(jnp.where(page_hits, entries[None, :] // cpages, 0), 1)
    page_slot = jnp.sum(jnp.where(page_hits, entries[None, :] % cpages, 0), 1)
    page_length = jnp.sum(
        jnp.where(page_prompt[:, None] == prompts[None, :], prompt_length[None, :], 0), 1
    )
    visible = (
        page_slot[:, None] * page_size + jnp.arange(page_size, dtype=jnp.int32)[None, :]
        < page_length[:, None]
    )
    pool_prompt = jnp.where(visible, page_prompt[:, None], -1).reshape(-1)
    key_prompt = jnp.concatenate([pool_prompt, jnp.repeat(prompt_owner, span)])
    key_table = jnp.concatenate([page_pool.reshape(-1, 2 * HD), arrived], 0)
    cached_keys = key_table[:, :HD]
    cached_values = key_table[:, HD:]
    scale = 1.0 / math.sqrt(HD)
    causal = jnp.arange(steps)[None, :] <= jnp.arange(steps)[:, None]
    per_block = max(1, min(rows, 512 // (steps * heads_dev)))
    blocks = rows // per_block
    queries = decode_queries.reshape(blocks, per_block, steps, heads_dev, HD)

    def attend(items):
        query, prompt, own_tail = items
        flat = query.reshape(-1, HD)
        scores = (
            lax.dot_general(
                flat, cached_keys, (((1,), (1,)), ((), ())), preferred_element_type=jnp.float32
            )
            * scale
        )
        scores = scores.reshape(per_block, steps, heads_dev, -1)
        allowed = (key_prompt[None, :] == prompt[:, None])[:, None, None, :]
        scores = jnp.where(allowed, scores, -jnp.inf)
        tail_scores = (
            jnp.einsum(
                "rshd,rtd->rsht", query, own_tail[..., :HD], preferred_element_type=jnp.float32
            )
            * scale
        )
        tail_scores = jnp.where(causal[None, :, None, :], tail_scores, -jnp.inf)
        highest = jnp.maximum(jnp.max(scores, -1), jnp.max(tail_scores, -1))
        weight = jnp.exp(scores - highest[..., None])
        tail_weight = jnp.exp(tail_scores - highest[..., None])
        total = jnp.sum(weight, -1) + jnp.sum(tail_weight, -1)
        rounded = weight.astype(jnp.bfloat16).reshape(-1, weight.shape[-1])
        mixed = jnp.dot(rounded, cached_values, preferred_element_type=jnp.float32).reshape(
            per_block, steps, heads_dev, HD
        )
        mixed = mixed + jnp.einsum(
            "rsht,rtd->rshd",
            tail_weight.astype(jnp.bfloat16),
            own_tail[..., HD:],
            preferred_element_type=jnp.float32,
        )
        return (mixed / total[..., None]).astype(jnp.bfloat16)

    attended = lax.map(
        attend,
        (
            queries,
            fork_map.reshape(blocks, per_block),
            tail_pair.reshape(blocks, per_block, steps, 2 * HD),
        ),
    )
    head_rows = attended.reshape(rows * steps, heads_dev * HD)
    decoded = jnp.dot(
        lax.all_gather(head_rows, "tensor", axis=1, tiled=True),
        out_weight,
        preferred_element_type=jnp.float32,
    )
    return decoded.astype(jnp.bfloat16).reshape(rows, steps, width)


MESH_ID = pl.DeviceIdType.MESH
TILE = 128
FAR = -(2.0**100)


def nt(left, right):
    return lax.dot_general(
        left, right, (((1,), (1,)), ((), ())), preferred_element_type=jnp.float32
    )


def fused(
    n, n_rep, steps, owner_s, length_s, table_s, fork, span_hbm, dec_hbm, query_hbm, wk_hbm,
    wv_hbm, w_hbm, pool_hbm, out,
    span_tok, dec_tok, query_in, query, w_kv, w_all, pool, hot, cosine, sine,
    part, own, landed, proj, hop_out, hop_in, keys, values, new_keys, new_values,
    mixed, top, gathered, acc,
    in_sem, sp_send, sp_recv, rs_send, rs_recv, nk_send, nk_recv, ag_send, ag_recv, re_send,
):
    z = lax.axis_index("tensor")
    rep = lax.axis_index("replica")
    bf16, f32 = jnp.bfloat16, jnp.float32
    span, depth = span_tok.shape
    rows = dec_tok.shape[0]
    number = rows * steps
    chunks = number // TILE
    group = TILE // steps
    width = query.shape[1]
    heads = width // HD
    pairs = heads // 2
    pages, page_size = pool.shape[0], pool.shape[1]
    cpages = pages // n_rep
    features = w_all.shape[1]
    two = 2 * HD
    factor = math.log2(math.e) / math.sqrt(HD)

    def at(block):
        if isinstance(block, int):
            return pl.ds(block * TILE, TILE)
        return pl.ds(pl.multiple_of(block * TILE, TILE), TILE)

    def load(src, dst, slot):
        return pltpu.make_async_copy(src, dst, in_sem.at[slot])

    loads = [load(span_hbm, span_tok, 0)]
    for d in range(n):
        column = pl.ds(d * HD, HD)
        loads.append(load(wk_hbm.at[:, column], w_kv.at[:, pl.ds(d * two, HD)], 1 + 2 * d))
        loads.append(load(wv_hbm.at[:, column], w_kv.at[:, pl.ds(d * two + HD, HD)], 2 + 2 * d))
    first_dec = len(loads)
    for c in range(chunks):
        piece = pl.ds(c * group, group)
        loads.append(load(dec_hbm.at[piece], dec_tok.at[piece], first_dec + c))
    pool_load = load(pool_hbm, pool, first_dec + chunks)
    query_load = load(query_hbm, query_in, first_dec + chunks + 1)
    w_load = load(w_hbm, w_all, first_dec + chunks + 2)
    for item in loads:
        item.start()
    pool_load.start()
    query_load.start()

    barrier = pltpu.get_barrier_semaphore()
    for k in range(1, n):
        pl.semaphore_signal(
            barrier, inc=1, device_id={"tensor": lax.rem(z + k, n)}, device_id_type=MESH_ID
        )
    for k in range(1, n_rep):
        pl.semaphore_signal(
            barrier, inc=1, device_id={"replica": lax.rem(rep + k, n_rep)}, device_id_type=MESH_ID
        )

    def turns(places, block):
        lane = lax.broadcasted_iota(jnp.int32, (TILE, HD), 1)
        half = HD // 2
        low = lane < half
        power = jnp.where(low, lane, lane - half).astype(f32) * (-(2.0 / HD) * math.log(rope_base))
        angle = places * jnp.exp(power)
        cosine[at(block), :] = jnp.cos(angle)
        turned = jnp.sin(angle)
        sine[at(block), :] = jnp.where(low, -turned, turned)

    own_length = length_s[owner_s[rep]]
    for block in range(span // TILE):
        line = lax.broadcasted_iota(jnp.int32, (TILE, HD), 0)
        turns((line + (own_length + block * TILE)).astype(f32), block)

    for item in loads[:first_dec]:
        item.wait()
    pl.semaphore_wait(barrier, n + n_rep - 2)
    for block in range(span // TILE):
        term = jnp.dot(span_tok[at(block), :], w_kv[...], preferred_element_type=f32)
        for d in range(n):
            part[d, at(block), :] = term[:, d * two : (d + 1) * two].astype(bf16)
            own[d, at(block), :] = term[:, d * two : (d + 1) * two]

    def ahead(side, distance):
        return z + distance if side == 0 else z - distance

    def behind(side, distance):
        return ahead(1 - side, distance)

    def on_line(place):
        return (place >= 0) & (place < n)

    def sp_copy(side, distance):
        target = ahead(side, distance)
        return pltpu.make_async_remote_copy(
            src_ref=part.at[target],
            dst_ref=landed.at[side, distance - 1],
            send_sem=sp_send.at[side, distance - 1],
            recv_sem=sp_recv.at[side, distance - 1],
            device_id={"tensor": target},
            device_id_type=MESH_ID,
        )

    def sp_arrival(side, distance):
        return pltpu.make_async_remote_copy(
            src_ref=part.at[0],
            dst_ref=landed.at[side, distance - 1],
            send_sem=sp_send.at[side, distance - 1],
            recv_sem=sp_recv.at[side, distance - 1],
            device_id={"tensor": lax.rem(z + 1, n)},
            device_id_type=MESH_ID,
        )

    for distance in range(n - 1, 0, -1):
        for side in (0, 1):

            @pl.when(on_line(ahead(side, distance)))
            def _():
                sp_copy(side, distance).start()

    w_load.start()

    def hop(side, c, d):
        return pltpu.make_async_remote_copy(
            src_ref=hop_out.at[side, c, d],
            dst_ref=hop_in.at[side, c, d],
            send_sem=rs_send.at[side, c, d],
            recv_sem=rs_recv.at[side, c, d],
            device_id={"tensor": jnp.clip(ahead(side, 1), 0, n - 1)},
            device_id_type=MESH_ID,
        )

    def onward(side):
        return range(n - 1, 0, -1) if side == 0 else range(0, n - 1)

    def beyond(side, d):
        return d > z if side == 0 else d < z

    def is_end(side):
        return z == 0 if side == 0 else z == n - 1

    def project(c):
        loads[first_dec + c].wait()
        tokens = dec_tok[pl.ds(c * group, group)].reshape(TILE, depth)
        term = jnp.dot(tokens, w_kv[...], preferred_element_type=f32)
        for d in range(n):
            proj[c, d] = term[:, d * two : (d + 1) * two]

        for side in (0, 1):

            @pl.when(is_end(side))
            def _():
                for d in onward(side):
                    hop_out[side, c, d] = proj[c, d].astype(bf16)
                    hop(side, c, d).start()

    def relay(c, side, node):
        @pl.when(z == node)
        def _():
            for d in onward(side):
                if (d > node) if side == 0 else (d < node):
                    hop(side, c, d).wait_recv()
                    total = proj[c, d] + hop_in[side, c, d].astype(f32)
                    hop_out[side, c, d] = total.astype(bf16)
                    hop(side, c, d).start()

    def relay_step(c, k):
        relay(c, 0, k)
        relay(c, 1, n - 1 - k)

    def rotate(total, block):
        key = total[:, :HD]
        key = key * cosine[at(block), :] + pltpu.roll(key, HD // 2, 1) * sine[at(block), :]
        return key.astype(bf16), total[:, HD:].astype(bf16)

    for c in range(chunks):
        project(c)

    prompt_of = lax.broadcasted_iota(jnp.int32, (HD, rows), 0)
    chosen = (prompt_of == fork[...]).astype(f32).astype(bf16)
    lanes = lax.broadcasted_iota(jnp.int32, (TILE, HD), 1)
    lines = lax.broadcasted_iota(jnp.int32, (TILE, HD), 0)
    lengths = jnp.zeros((TILE, HD), f32)
    for p in range(n_rep):
        lengths = jnp.where(lanes == p, length_s[p].astype(f32), lengths)
    for c in range(chunks):
        line = lax.broadcasted_iota(jnp.int32, (TILE, rows), 0)
        lane = lax.broadcasted_iota(jnp.int32, (TILE, rows), 1)
        belongs = (line // steps + c * group == lane).astype(f32).astype(bf16)
        one_hot = nt(belongs, chosen)
        hot[at(c), :] = one_hot.astype(bf16)
        length = jnp.sum(one_hot * lengths, 1, keepdims=True)
        turns(length + (lines % steps + span).astype(f32), c + span // TILE)

    pool_load.wait()
    for j in range(pages):
        p = j // cpages
        start = (j % cpages) * page_size
        place = pl.ds(j * page_size, page_size)
        page = pool[table_s[j]]
        line = lax.broadcasted_iota(jnp.int32, (page_size, HD), 0)
        lane = lax.broadcasted_iota(jnp.int32, (page_size, HD), 1)
        seen = (lane == p) & (line + start < length_s[p])
        keys[place, :HD] = page[:, :HD]
        keys[place, HD:] = jnp.where((lane >= n_rep) | seen, 0.0, FAR).astype(bf16)
        values[place, :HD] = page[:, HD:]
        values[place, HD:] = jnp.ones((page_size, HD), bf16)

    fresh = n_rep * span
    for r in range(n_rep):
        lane = lax.broadcasted_iota(jnp.int32, (span, HD), 1)
        place = pl.ds(r * span, span)
        near = (lane >= n_rep) | (lane == owner_s[r])
        new_keys[place, HD:] = jnp.where(near, 0.0, FAR).astype(bf16)
    new_keys[pl.ds(fresh, TILE), HD:] = jnp.zeros((TILE, HD), bf16)
    new_values[:, HD:] = jnp.ones((new_values.shape[0], HD), bf16)

    query_load.wait()
    for c in range(chunks):
        query[at(c), :] = query_in[pl.ds(c * group, group)].reshape(TILE, width)

    def asked(c, pair):
        asks = []
        for k in range(2):
            column = pl.ds(pl.multiple_of((2 * pair + k) * HD, HD), HD)
            asks.append(jnp.concatenate([query[at(c), column], hot[at(c), :]], 1))
        return jnp.concatenate(asks, 0)

    def cached_part(c):
        @pl.loop(0, pairs)
        def _(pair):
            scores = nt(asked(c, pair), keys[...])
            highest = jnp.max(scores, 1, keepdims=True)
            weight = jnp.exp2((scores - highest) * factor).astype(bf16)
            mixed[c * pairs + pair] = jnp.dot(weight, values[...], preferred_element_type=f32)
            top[c * pairs + pair] = jnp.broadcast_to(highest, (2 * TILE, HD))

    def nk_copy(array, kind, k, whose):
        place = pl.ds(pl.multiple_of(whose * span, span), span)
        return pltpu.make_async_remote_copy(
            src_ref=array.at[place, pl.ds(0, HD)],
            dst_ref=array.at[place, pl.ds(0, HD)],
            send_sem=nk_send.at[kind, k - 1],
            recv_sem=nk_recv.at[kind, k - 1],
            device_id={"replica": lax.rem(rep + k, n_rep)},
            device_id_type=MESH_ID,
        )

    def finish_span():
        for side in (0, 1):
            for distance in range(1, n):

                @pl.when(on_line(behind(side, distance)))
                def _():
                    sp_arrival(side, distance).wait_recv()
                    own[z] = own[z] + landed[side, distance - 1].astype(f32)

        for block in range(span // TILE):
            key, value = rotate(own[z, at(block), :], block)
            place = pl.ds(pl.multiple_of(rep * span + block * TILE, TILE), TILE)
            new_keys[place, :HD] = key
            new_values[place, :HD] = value
        for k in range(1, n_rep):
            nk_copy(new_keys, 0, k, rep).start()
            nk_copy(new_values, 1, k, rep).start()

    def wait_span():
        for k in range(1, n_rep):
            whose = lax.rem(rep - k + n_rep, n_rep)
            nk_copy(new_keys, 0, k, whose).wait_recv()
            nk_copy(new_values, 1, k, whose).wait_recv()

    def finish_tail(c):
        for side in (0, 1):

            @pl.when(jnp.logical_not(is_end(side)))
            def _():
                for d in range(n):

                    @pl.when(z == d)
                    def _():
                        if d != (0 if side == 0 else n - 1):
                            hop(side, c, d).wait_recv()
                            proj[c, d] = proj[c, d] + hop_in[side, c, d].astype(f32)

        key, value = rotate(proj[c, z], c + span // TILE)
        new_keys[pl.ds(fresh, TILE), :HD] = key
        new_values[pl.ds(fresh, TILE), :HD] = value

    half_heads = width // 2

    def block_of(origin, c, half):
        column = pl.ds(half * half_heads, half_heads)
        return gathered.at[origin, at(c), column]

    def ag_copy(side, distance, c, half):
        return pltpu.make_async_remote_copy(
            src_ref=block_of(z, c, half),
            dst_ref=block_of(z, c, half),
            send_sem=ag_send.at[side, distance - 1, c, half],
            recv_sem=ag_recv.at[side, distance - 1, c, half],
            device_id={"tensor": jnp.clip(ahead(side, distance), 0, n - 1)},
            device_id_type=MESH_ID,
        )

    def ag_relay(side, distance, c, half):
        origin = behind(side, distance)
        return pltpu.make_async_remote_copy(
            src_ref=block_of(origin, c, half),
            dst_ref=block_of(origin, c, half),
            send_sem=re_send.at[side, distance - 1, c, half],
            recv_sem=ag_recv.at[side, distance, c, half],
            device_id={"tensor": jnp.clip(ahead(side, 1), 0, n - 1)},
            device_id_type=MESH_ID,
        )

    def ag_arrival(side, distance, c, half):
        origin = behind(side, distance)
        return pltpu.make_async_remote_copy(
            src_ref=block_of(origin, c, half),
            dst_ref=block_of(origin, c, half),
            send_sem=ag_send.at[side, 0, c, half],
            recv_sem=ag_recv.at[side, distance - 1, c, half],
            device_id={"tensor": jnp.clip(ahead(side, 1), 0, n - 1)},
            device_id_type=MESH_ID,
        )

    def sends_to(side, distance):
        place = ahead(side, distance)
        inner = (place <= n - 2) if side == 0 else (place >= 1)
        if distance == 1:
            inner = inner | ((z == n - 2) if side == 0 else (z == 1))
        return inner & on_line(place)

    def relays(side):
        return (z == n - 2) if side == 0 else (z == 1)

    causal_line = lax.broadcasted_iota(jnp.int32, (2 * TILE, TILE), 0)
    causal_lane = lax.broadcasted_iota(jnp.int32, (2 * TILE, TILE), 1)
    causal_line = jnp.where(causal_line >= TILE, causal_line - TILE, causal_line)
    causal = (causal_line // steps == causal_lane // steps) & (causal_lane <= causal_line)

    def new_part(c):
        for half in range(2):

            @pl.loop(half * (pairs // 2), (half + 1) * (pairs // 2))
            def _(pair):
                scores = nt(asked(c, pair), new_keys[...])
                plain = scores[:, :fresh]
                tail = jnp.where(causal, scores[:, fresh:], FAR)
                before = top[c * pairs + pair][:, :1]
                highest = jnp.maximum(
                    jnp.maximum(before, jnp.max(plain, 1, keepdims=True)),
                    jnp.max(tail, 1, keepdims=True),
                )
                weight = jnp.exp2((plain - highest) * factor).astype(bf16)
                tail_weight = jnp.exp2((tail - highest) * factor).astype(bf16)
                weight = jnp.concatenate([weight, tail_weight], 1)
                total = mixed[c * pairs + pair] * jnp.exp2((before - highest) * factor)
                total = total + jnp.dot(weight, new_values[...], preferred_element_type=f32)
                result = (total[:, :HD] / total[:, HD:]).astype(bf16)
                for k in range(2):
                    column = pl.ds(pl.multiple_of((2 * pair + k) * HD, HD), HD)
                    gathered[z, at(c), column] = result[k * TILE : (k + 1) * TILE]

            for distance in range(max(1, n - 2), 0, -1):
                for side in (0, 1):

                    @pl.when(sends_to(side, distance))
                    def _():
                        ag_copy(side, distance, c, half).start()

    cached_part(0)
    for k in range(1, n - 1):
        relay_step(0, k)
    finish_span()
    for c in range(1, chunks):
        cached_part(c)
        for k in range(1, n - 1):
            relay_step(c, k)
    wait_span()
    for c in range(chunks):
        finish_tail(c)
        new_part(c)

    w_load.wait()
    wide = min(512, features)

    def add(origin, block, size, first, last):
        place = pl.ds(pl.multiple_of(block * size, size), size)
        deep = pl.ds(pl.multiple_of(origin * width, width), width)

        @pl.loop(0, features // wide)
        def _(column):
            cols = pl.ds(pl.multiple_of(column * wide, wide), wide)
            term = jnp.dot(
                gathered[origin, place, :], w_all[deep, cols], preferred_element_type=f32
            )
            if first:
                acc[place, cols] = term
            else:
                acc[place, cols] += term

    tall = min(2 * TILE, number)

    @pl.loop(0, number // tall)
    def _(block):
        add(z, block, tall, True, False)

    @pl.loop(0, chunks)
    def _(c):
        for distance in range(1, n):
            for side in (0, 1):

                @pl.when(on_line(behind(side, distance)))
                def _():
                    for half in range(2):
                        ag_arrival(side, distance, c, half).wait_recv()
                        if distance < n - 1:

                            @pl.when(relays(side))
                            def _():
                                ag_relay(side, distance, c, half).start()

                    add(behind(side, distance), c, TILE, False, False)

        place = pl.ds(c * group, group)

        @pl.loop(0, features // wide)
        def _(column):
            cols = pl.ds(pl.multiple_of(column * wide, wide), wide)
            done = acc[at(c), cols].astype(bf16)
            out[place, :, cols] = done.reshape(group, steps, wide)

    for distance in range(1, n):
        for side in (0, 1):

            @pl.when(on_line(ahead(side, distance)))
            def _():
                sp_copy(side, distance).wait_send()

    for k in range(1, n_rep):
        nk_copy(new_keys, 0, k, rep).wait_send()
        nk_copy(new_values, 1, k, rep).wait_send()
    for side in (0, 1):
        for d in onward(side):

            @pl.when(beyond(side, d))
            def _():
                @pl.loop(0, chunks)
                def _(c):
                    hop(side, c, d).wait_send()

        for distance in range(1, max(2, n - 1)):

            @pl.when(sends_to(side, distance))
            def _():
                @pl.loop(0, chunks)
                def _(c):
                    for half in range(2):
                        ag_copy(side, distance, c, half).wait_send()

        for distance in range(1, n - 1):

            @pl.when(relays(side) & on_line(behind(side, distance)))
            def _():
                @pl.loop(0, chunks)
                def _(c):
                    for half in range(2):
                        ag_relay(side, distance, c, half).wait_send()


def on_device(
    prompt_owner,
    fork_map,
    page_table,
    prompt_length,
    span_states,
    decode_states,
    decode_queries,
    key_weight,
    value_weight,
    out_weight,
    page_pool,
):
    n_replica = lax.axis_size("replica")
    n_tensor = lax.axis_size("tensor")
    span = span_states.shape[0]
    rows, steps, width = decode_states.shape
    heads_width = decode_queries.shape[2]
    heads_dev = heads_width // HD
    kv_heads = key_weight.shape[1] // HD
    number = rows * steps
    if (
        kv_heads != n_tensor
        or n_tensor < 2
        or n_replica < 2
        or span % TILE
        or number % TILE
        or number % min(2 * TILE, number)
        or TILE % steps
        or heads_dev % 4
        or n_replica > HD
    ):
        return general(
            prompt_owner, fork_map, page_table, prompt_length, span_states, decode_states,
            decode_queries, key_weight, value_weight, out_weight, page_pool,
        )
    features = out_weight.shape[1]
    pages, page_size = page_pool.shape[1], page_pool.shape[2]
    cached = pages * page_size
    fresh = n_replica * span + TILE
    chunks = number // TILE
    two = 2 * HD
    pairs = chunks * heads_dev // 2
    inner = max(1, n_tensor - 2)
    bf16, f32 = jnp.bfloat16, jnp.float32
    dma = pltpu.SemaphoreType.DMA
    vmem, smem = pltpu.VMEM, pl.BlockSpec(memory_space=pltpu.SMEM)
    whole = pl.BlockSpec(memory_space=pltpu.VMEM)
    return pl.pallas_call(
        functools.partial(fused, n_tensor, n_replica, steps),
        name="fused",
        out_shape=jax.ShapeDtypeStruct((rows, steps, features), bf16),
        in_specs=[smem] * 3 + [whole] + [pl.BlockSpec(memory_space=pl.ANY)] * 7,
        out_specs=whole,
        scratch_shapes=[
            vmem(span_states.shape, bf16),
            vmem(decode_states.shape, bf16),
            vmem(decode_queries.shape, bf16),
            vmem((number, heads_width), bf16),
            vmem((width, n_tensor * two), bf16),
            vmem(out_weight.shape, bf16),
            vmem(page_pool.shape[1:], bf16),
            vmem((number, HD), bf16),
            vmem((span + number, HD), f32),
            vmem((span + number, HD), f32),
            vmem((n_tensor, span, two), bf16),
            vmem((n_tensor, span, two), f32),
            vmem((2, n_tensor - 1, span, two), bf16),
            vmem((chunks, n_tensor, TILE, two), f32),
            vmem((2, chunks, n_tensor, TILE, two), bf16),
            vmem((2, chunks, n_tensor, TILE, two), bf16),
            vmem((cached, two), bf16),
            vmem((cached, two), bf16),
            vmem((fresh, two), bf16),
            vmem((fresh, two), bf16),
            vmem((pairs, 2 * TILE, two), f32),
            vmem((pairs, 2 * TILE, HD), f32),
            vmem((n_tensor, number, heads_width), bf16),
            vmem((number, features), f32),
            dma((2 * n_tensor + chunks + 4,)),
            dma((2, n_tensor - 1)),
            dma((2, n_tensor - 1)),
            dma((2, chunks, n_tensor)),
            dma((2, chunks, n_tensor)),
            dma((2, n_replica - 1)),
            dma((2, n_replica - 1)),
            dma((2, inner, chunks, 2)),
            dma((2, n_tensor - 1, chunks, 2)),
            dma((2, inner, chunks, 2)),
        ],
        compiler_params=pltpu.CompilerParams(
            collective_id=0, has_side_effects=True, vmem_limit_bytes=62 * 1024 * 1024
        ),
    )(
        prompt_owner, prompt_length, page_table, fork_map.reshape(1, rows), span_states,
        decode_states, decode_queries, key_weight, value_weight, out_weight,
        page_pool.reshape(page_pool.shape[1:]),
    )


def solution(mesh):
    in_specs = (
        P("parts"),
        P(("parts", "replica")),
        P("parts"),
        P("parts"),
        P(("parts", "replica"), "tensor"),
        P(("parts", "replica"), None, "tensor"),
        P(("parts", "replica"), None, "tensor"),
        P("tensor", None),
        P("tensor", None),
        P(None, "tensor"),
        P("tensor", "parts", None, None),
    )
    out_specs = P(("parts", "replica"), None, "tensor")
    return jax.shard_map(
        on_device, mesh=mesh, in_specs=in_specs, out_specs=out_specs, check_vma=False
    )
```

```python
import functools
import math

import jax
import jax.numpy as jnp
from jax import lax
from jax.experimental import pallas as pl
from jax.experimental.pallas import tpu as pltpu
from jax.sharding import PartitionSpec as P

HD = 128


rope_base = 1000000.0


def rotary(vectors, places):
    half = vectors.shape[-1] // 2
    freq = rope_base ** (-(2.0 / vectors.shape[-1]) * jnp.arange(half, dtype=jnp.float32))
    angle = places.astype(jnp.float32)[..., None, None] * freq
    cosine = jnp.cos(angle)
    sine = jnp.sin(angle)
    first = vectors[..., :half]
    second = vectors[..., half:]
    return jnp.concatenate([first * cosine - second * sine, second * cosine + first * sine], -1)


def rotate_round(summed, places, kv_heads):
    number = summed.shape[0]
    turned = rotary(summed[:, : kv_heads * HD].reshape(number, kv_heads, HD), places)
    turned = turned.astype(jnp.bfloat16).reshape(number, kv_heads * HD)
    return jnp.concatenate([turned, summed[:, kv_heads * HD :].astype(jnp.bfloat16)], 1)


def own_pair(packed, head_group, kv_heads):
    key_part = lax.dynamic_slice_in_dim(packed, head_group * HD, HD, 1)
    value_part = lax.dynamic_slice_in_dim(packed, (kv_heads + head_group) * HD, HD, 1)
    return jnp.concatenate([key_part, value_part], 1)


def general(
    prompt_owner,
    fork_map,
    page_table,
    prompt_length,
    span_states,
    decode_states,
    decode_queries,
    key_weight,
    value_weight,
    out_weight,
    page_pool,
):
    replica = lax.axis_index("replica")
    device_rank = lax.axis_index("tensor")
    n_replica = lax.axis_size("replica")
    n_tensor = lax.axis_size("tensor")
    span = span_states.shape[0]
    rows, steps, width = decode_states.shape
    heads_dev = decode_queries.shape[2] // HD
    kv_heads = key_weight.shape[1] // HD
    sharing = n_tensor // kv_heads
    prompts = jnp.arange(n_replica, dtype=jnp.int32)
    own_prompt = jnp.sum(jnp.where(prompts == replica, prompt_owner, 0))
    own_length = jnp.sum(jnp.where(prompts == own_prompt, prompt_length, 0))
    row_hits = fork_map[:, None] == prompts[None, :]
    row_length = jnp.sum(jnp.where(row_hits, prompt_length[None, :], 0), 1)
    positions = jnp.concatenate(
        [
            own_length + jnp.arange(span, dtype=jnp.int32),
            (row_length[:, None] + span + jnp.arange(steps, dtype=jnp.int32)[None, :]).reshape(-1),
        ]
    )
    tokens = jnp.concatenate([span_states, decode_states.reshape(rows * steps, width)], 0)
    projected = jnp.dot(
        tokens, jnp.concatenate([key_weight, value_weight], 1), preferred_element_type=jnp.float32
    )
    share = lax.psum_scatter(projected, "tensor", scatter_dimension=0, tiled=True)
    number = share.shape[0]
    start = device_rank * number
    places = lax.dynamic_slice_in_dim(positions, start, number)
    turned = rotate_round(share, places, kv_heads)
    groups = jnp.stack(
        [own_pair(turned, group_index, kv_heads) for group_index in range(kv_heads)], 0
    )
    outgoing = jnp.repeat(groups, sharing, axis=0)
    paired = lax.all_to_all(outgoing, "tensor", split_axis=0, concat_axis=1, tiled=True).reshape(
        -1, 2 * HD
    )
    arrived = lax.all_gather(paired[:span], "replica", axis=0, tiled=True)
    tail_pair = paired[span:].reshape(rows, steps, 2 * HD)
    pool_pages = page_table.shape[0]
    cpages = pool_pages // n_replica
    page_size = page_pool.shape[2]
    entries = jnp.arange(pool_pages, dtype=jnp.int32)
    page_hits = page_table[None, :] == entries[:, None]
    page_prompt = jnp.sum(jnp.where(page_hits, entries[None, :] // cpages, 0), 1)
    page_slot = jnp.sum(jnp.where(page_hits, entries[None, :] % cpages, 0), 1)
    page_length = jnp.sum(
        jnp.where(page_prompt[:, None] == prompts[None, :], prompt_length[None, :], 0), 1
    )
    visible = (
        page_slot[:, None] * page_size + jnp.arange(page_size, dtype=jnp.int32)[None, :]
        < page_length[:, None]
    )
    pool_prompt = jnp.where(visible, page_prompt[:, None], -1).reshape(-1)
    key_prompt = jnp.concatenate([pool_prompt, jnp.repeat(prompt_owner, span)])
    key_table = jnp.concatenate([page_pool.reshape(-1, 2 * HD), arrived], 0)
    cached_keys = key_table[:, :HD]
    cached_values = key_table[:, HD:]
    scale = 1.0 / math.sqrt(HD)
    causal = jnp.arange(steps)[None, :] <= jnp.arange(steps)[:, None]
    per_block = max(1, min(rows, 512 // (steps * heads_dev)))
    blocks = rows // per_block
    queries = decode_queries.reshape(blocks, per_block, steps, heads_dev, HD)

    def attend(items):
        query, prompt, own_tail = items
        flat = query.reshape(-1, HD)
        scores = (
            lax.dot_general(
                flat, cached_keys, (((1,), (1,)), ((), ())), preferred_element_type=jnp.float32
            )
            * scale
        )
        scores = scores.reshape(per_block, steps, heads_dev, -1)
        allowed = (key_prompt[None, :] == prompt[:, None])[:, None, None, :]
        scores = jnp.where(allowed, scores, -jnp.inf)
        tail_scores = (
            jnp.einsum(
                "rshd,rtd->rsht", query, own_tail[..., :HD], preferred_element_type=jnp.float32
            )
            * scale
        )
        tail_scores = jnp.where(causal[None, :, None, :], tail_scores, -jnp.inf)
        highest = jnp.maximum(jnp.max(scores, -1), jnp.max(tail_scores, -1))
        weight = jnp.exp(scores - highest[..., None])
        tail_weight = jnp.exp(tail_scores - highest[..., None])
        total = jnp.sum(weight, -1) + jnp.sum(tail_weight, -1)
        rounded = weight.astype(jnp.bfloat16).reshape(-1, weight.shape[-1])
        mixed = jnp.dot(rounded, cached_values, preferred_element_type=jnp.float32).reshape(
            per_block, steps, heads_dev, HD
        )
        mixed = mixed + jnp.einsum(
            "rsht,rtd->rshd",
            tail_weight.astype(jnp.bfloat16),
            own_tail[..., HD:],
            preferred_element_type=jnp.float32,
        )
        return (mixed / total[..., None]).astype(jnp.bfloat16)

    attended = lax.map(
        attend,
        (
            queries,
            fork_map.reshape(blocks, per_block),
            tail_pair.reshape(blocks, per_block, steps, 2 * HD),
        ),
    )
    head_rows = attended.reshape(rows * steps, heads_dev * HD)
    decoded = jnp.dot(
        lax.all_gather(head_rows, "tensor", axis=1, tiled=True),
        out_weight,
        preferred_element_type=jnp.float32,
    )
    return decoded.astype(jnp.bfloat16).reshape(rows, steps, width)


MESH_ID = pl.DeviceIdType.MESH
TILE = 128
FAR = -(2.0**100)


def nt(left, right):
    return lax.dot_general(
        left, right, (((1,), (1,)), ((), ())), preferred_element_type=jnp.float32
    )


def fused(
    n, n_rep, steps, owner_s, length_s, table_s, fork, span_hbm, dec_hbm, query_hbm, wk_hbm,
    wv_hbm, w_hbm, pool_hbm, out,
    span_tok, dec_tok, query_in, query, w_kv, w_all, pool, hot, cosine, sine,
    part, own, landed, hop_out, hop_in, keys, values, new_keys, new_values,
    mixed, top, gathered, acc, result,
    in_sem, sp_send, sp_recv, rs_send, rs_recv, nk_send, nk_recv, ag_send, ag_recv, re_send, out_sem,
):
    z = lax.axis_index("tensor")
    rep = lax.axis_index("replica")
    bf16, f32 = jnp.bfloat16, jnp.float32
    span, depth = span_tok.shape
    rows = dec_tok.shape[0]
    number = rows * steps
    chunks = number // TILE
    group = TILE // steps
    width = query.shape[1]
    heads = width // HD
    pairs = heads // 2
    pages, page_size = pool.shape[0], pool.shape[1]
    cpages = pages // n_rep
    features = w_all.shape[1]
    two = 2 * HD
    factor = math.log2(math.e) / math.sqrt(HD)

    def at(block):
        if isinstance(block, int):
            return pl.ds(block * TILE, TILE)
        return pl.ds(pl.multiple_of(block * TILE, TILE), TILE)

    def load(src, dst, slot):
        return pltpu.make_async_copy(src, dst, in_sem.at[slot])

    loads = [load(span_hbm, span_tok, 0)]
    for d in range(n):
        column = pl.ds(d * HD, HD)
        loads.append(load(wk_hbm.at[:, column], w_kv.at[:, pl.ds(d * two, HD)], 1 + 2 * d))
        loads.append(load(wv_hbm.at[:, column], w_kv.at[:, pl.ds(d * two + HD, HD)], 2 + 2 * d))
    first_dec = len(loads)
    for c in range(chunks):
        piece = pl.ds(c * group, group)
        loads.append(load(dec_hbm.at[piece], dec_tok.at[piece], first_dec + c))
    pool_load = load(pool_hbm, pool, first_dec + chunks)
    query_load = load(query_hbm, query_in, first_dec + chunks + 1)
    w_load = load(w_hbm, w_all, first_dec + chunks + 2)
    for item in loads:
        item.start()
    pool_load.start()
    query_load.start()

    barrier = pltpu.get_barrier_semaphore()
    for k in range(1, n):
        pl.semaphore_signal(
            barrier, inc=1, device_id={"tensor": lax.rem(z + k, n)}, device_id_type=MESH_ID
        )
    for k in range(1, n_rep):
        pl.semaphore_signal(
            barrier, inc=1, device_id={"replica": lax.rem(rep + k, n_rep)}, device_id_type=MESH_ID
        )

    def turns(places, block):
        lane = lax.broadcasted_iota(jnp.int32, (TILE, HD), 1)
        half = HD // 2
        low = lane < half
        power = jnp.where(low, lane, lane - half).astype(f32) * (-(2.0 / HD) * math.log(rope_base))
        angle = places * jnp.exp(power)
        cosine[at(block), :] = jnp.cos(angle)
        turned = jnp.sin(angle)
        sine[at(block), :] = jnp.where(low, -turned, turned)

    own_length = length_s[owner_s[rep]]
    for block in range(span // TILE):
        line = lax.broadcasted_iota(jnp.int32, (TILE, HD), 0)
        turns((line + (own_length + block * TILE)).astype(f32), block)

    for item in loads[:first_dec]:
        item.wait()
    pl.semaphore_wait(barrier, n + n_rep - 2)
    def keep(kind, block, tokens):
        term = jnp.dot(tokens, w_kv[...], preferred_element_type=f32)
        for d in range(n):
            part[kind, d, at(block), :] = term[:, d * two : (d + 1) * two].astype(bf16)
            own[kind, d, at(block), :] = term[:, d * two : (d + 1) * two]

    for block in range(span // TILE):
        keep(0, block, span_tok[at(block), :])

    def ahead(side, distance):
        return z + distance if side == 0 else z - distance

    def behind(side, distance):
        return ahead(1 - side, distance)

    def on_line(place):
        return (place >= 0) & (place < n)

    def sized(kind):
        return pl.ds(0, span if kind == 0 else TILE)

    def sp_copy(kind, side, distance):
        target = ahead(side, distance)
        return pltpu.make_async_remote_copy(
            src_ref=part.at[kind, target, sized(kind)],
            dst_ref=landed.at[kind, side, distance - 1, sized(kind)],
            send_sem=sp_send.at[kind, side, distance - 1],
            recv_sem=sp_recv.at[kind, side, distance - 1],
            device_id={"tensor": target},
            device_id_type=MESH_ID,
        )

    def sp_arrival(kind, side, distance):
        return pltpu.make_async_remote_copy(
            src_ref=part.at[kind, 0, sized(kind)],
            dst_ref=landed.at[kind, side, distance - 1, sized(kind)],
            send_sem=sp_send.at[kind, side, distance - 1],
            recv_sem=sp_recv.at[kind, side, distance - 1],
            device_id={"tensor": lax.rem(z + 1, n)},
            device_id_type=MESH_ID,
        )

    def direct(kind, side, distance):
        place = ahead(side, distance)
        if kind < 2:
            return on_line(place)
        return (place >= 1) & (place <= n - 2)

    def scatter(kind):
        for distance in range(n - 1, 0, -1):
            for side in (0, 1):

                @pl.when(direct(kind, side, distance))
                def _():
                    sp_copy(kind, side, distance).start()

    def collect(kind):
        for side in (0, 1):
            for distance in range(1, n):

                arrives = on_line(behind(side, distance))
                if kind >= 2:
                    arrives = arrives & (z >= 1) & (z <= n - 2)

                @pl.when(arrives)
                def _():
                    sp_arrival(kind, side, distance).wait_recv()
                    own[kind, z, sized(kind)] = own[kind, z, sized(kind)] + landed[
                        kind, side, distance - 1, sized(kind)
                    ].astype(f32)

    def decode_tokens(c):
        loads[first_dec + c].wait()
        return dec_tok[pl.ds(c * group, group)].reshape(TILE, depth)

    scatter(0)
    keep(1, 0, decode_tokens(0))
    scatter(1)
    w_load.start()

    def hop(side, c):
        return pltpu.make_async_remote_copy(
            src_ref=hop_out.at[side, c - 1],
            dst_ref=hop_in.at[side, c - 1],
            send_sem=rs_send.at[side, c - 1],
            recv_sem=rs_recv.at[side, c - 1],
            device_id={"tensor": jnp.clip(ahead(side, 1), 0, n - 1)},
            device_id_type=MESH_ID,
        )

    def last(side):
        return n - 1 if side == 0 else 0

    def is_end(side):
        return z == 0 if side == 0 else z == n - 1

    def hop_on(side, c, total):
        hop_out[side, c - 1] = total.astype(bf16)
        hop(side, c).start()

    def project(c):
        keep(c + 1, 0, decode_tokens(c))
        for side in (0, 1):

            @pl.when(is_end(side))
            def _():
                hop_on(side, c, own[c + 1, last(side), sized(c + 1)])

    def relay_step(c, k):
        for side, node in ((0, k), (1, n - 1 - k)):

            @pl.when(z == node)
            def _():
                hop(side, c).wait_recv()
                total = own[c + 1, last(side), sized(c + 1)] + hop_in[side, c - 1].astype(f32)
                hop_on(side, c, total)

    def rotate(total, block):
        key = total[:, :HD]
        key = key * cosine[at(block), :] + pltpu.roll(key, HD // 2, 1) * sine[at(block), :]
        return key.astype(bf16), total[:, HD:].astype(bf16)

    for c in range(1, chunks):
        project(c)
    for c in range(1, chunks):
        scatter(c + 1)

    prompt_of = lax.broadcasted_iota(jnp.int32, (HD, rows), 0)
    chosen = (prompt_of == fork[...]).astype(f32).astype(bf16)
    lanes = lax.broadcasted_iota(jnp.int32, (TILE, HD), 1)
    lines = lax.broadcasted_iota(jnp.int32, (TILE, HD), 0)
    lengths = jnp.zeros((TILE, HD), f32)
    for p in range(n_rep):
        lengths = jnp.where(lanes == p, length_s[p].astype(f32), lengths)
    for c in range(chunks):
        line = lax.broadcasted_iota(jnp.int32, (TILE, rows), 0)
        lane = lax.broadcasted_iota(jnp.int32, (TILE, rows), 1)
        belongs = (line // steps + c * group == lane).astype(f32).astype(bf16)
        one_hot = nt(belongs, chosen)
        hot[at(c), :] = one_hot.astype(bf16)
        length = jnp.sum(one_hot * lengths, 1, keepdims=True)
        turns(length + (lines % steps + span).astype(f32), c + span // TILE)

    pool_load.wait()
    for j in range(pages):
        p = j // cpages
        start = (j % cpages) * page_size
        place = pl.ds(j * page_size, page_size)
        page = pool[table_s[j]]
        line = lax.broadcasted_iota(jnp.int32, (page_size, HD), 0)
        lane = lax.broadcasted_iota(jnp.int32, (page_size, HD), 1)
        seen = (lane == p) & (line + start < length_s[p])
        keys[place, :HD] = page[:, :HD]
        keys[place, HD:] = jnp.where((lane >= n_rep) | seen, 0.0, FAR).astype(bf16)
        values[place, :HD] = page[:, HD:]
        values[place, HD:] = jnp.ones((page_size, HD), bf16)

    fresh = n_rep * span
    for r in range(n_rep):
        lane = lax.broadcasted_iota(jnp.int32, (span, HD), 1)
        place = pl.ds(r * span, span)
        near = (lane >= n_rep) | (lane == owner_s[r])
        new_keys[place, HD:] = jnp.where(near, 0.0, FAR).astype(bf16)
    new_keys[pl.ds(fresh, TILE), HD:] = jnp.zeros((TILE, HD), bf16)
    new_values[:, HD:] = jnp.ones((new_values.shape[0], HD), bf16)

    query_load.wait()
    for c in range(chunks):
        query[at(c), :] = query_in[pl.ds(c * group, group)].reshape(TILE, width)

    def asked(c, pair):
        asks = []
        for k in range(2):
            column = pl.ds((2 * pair + k) * HD, HD)
            asks.append(jnp.concatenate([query[at(c), column], hot[at(c), :]], 1))
        return jnp.concatenate(asks, 0)

    def cached_part(c):
        for pair in range(pairs):
            scores = nt(asked(c, pair), keys[...])
            highest = jnp.max(scores, 1, keepdims=True)
            weight = jnp.exp2((scores - highest) * factor).astype(bf16)
            mixed[c * pairs + pair] = jnp.dot(weight, values[...], preferred_element_type=f32)
            top[c * pairs + pair] = jnp.broadcast_to(highest, (2 * TILE, HD))

    def nk_copy(array, kind, k, whose):
        place = pl.ds(pl.multiple_of(whose * span, span), span)
        return pltpu.make_async_remote_copy(
            src_ref=array.at[place, pl.ds(0, HD)],
            dst_ref=array.at[place, pl.ds(0, HD)],
            send_sem=nk_send.at[kind, k - 1],
            recv_sem=nk_recv.at[kind, k - 1],
            device_id={"replica": lax.rem(rep + k, n_rep)},
            device_id_type=MESH_ID,
        )

    def finish_span():
        collect(0)
        for block in range(span // TILE):
            key, value = rotate(own[0, z, at(block), :], block)
            place = pl.ds(pl.multiple_of(rep * span + block * TILE, TILE), TILE)
            new_keys[place, :HD] = key
            new_values[place, :HD] = value
        for k in range(1, n_rep):
            nk_copy(new_keys, 0, k, rep).start()
            nk_copy(new_values, 1, k, rep).start()

    def wait_span():
        for k in range(1, n_rep):
            whose = lax.rem(rep - k + n_rep, n_rep)
            nk_copy(new_keys, 0, k, whose).wait_recv()
            nk_copy(new_values, 1, k, whose).wait_recv()

    def place_tail(total, c):
        key, value = rotate(total, c + span // TILE)
        new_keys[pl.ds(fresh, TILE), :HD] = key
        new_values[pl.ds(fresh, TILE), :HD] = value

    def finish_tail(c):
        collect(c + 1)
        if c > 0:
            for side in (0, 1):

                @pl.when(z == last(side))
                def _():
                    hop(side, c).wait_recv()
                    own[c + 1, z, sized(c + 1)] = own[c + 1, z, sized(c + 1)] + hop_in[
                        side, c - 1
                    ].astype(f32)

        place_tail(own[c + 1, z, sized(c + 1)], c)

    half_heads = width // 2

    def block_of(origin, c, half):
        column = pl.ds(half * half_heads, half_heads)
        return gathered.at[origin, at(c), column]

    def ag_copy(side, distance, c, half):
        return pltpu.make_async_remote_copy(
            src_ref=block_of(z, c, half),
            dst_ref=block_of(z, c, half),
            send_sem=ag_send.at[side, distance - 1, c, half],
            recv_sem=ag_recv.at[side, distance - 1, c, half],
            device_id={"tensor": jnp.clip(ahead(side, distance), 0, n - 1)},
            device_id_type=MESH_ID,
        )

    def ag_relay(side, distance, c, half):
        origin = behind(side, distance)
        return pltpu.make_async_remote_copy(
            src_ref=block_of(origin, c, half),
            dst_ref=block_of(origin, c, half),
            send_sem=re_send.at[side, distance - 1, c, half],
            recv_sem=ag_recv.at[side, distance, c, half],
            device_id={"tensor": jnp.clip(ahead(side, 1), 0, n - 1)},
            device_id_type=MESH_ID,
        )

    def ag_arrival(side, distance, c, half):
        origin = behind(side, distance)
        return pltpu.make_async_remote_copy(
            src_ref=block_of(origin, c, half),
            dst_ref=block_of(origin, c, half),
            send_sem=ag_send.at[side, 0, c, half],
            recv_sem=ag_recv.at[side, distance - 1, c, half],
            device_id={"tensor": jnp.clip(ahead(side, 1), 0, n - 1)},
            device_id_type=MESH_ID,
        )

    def sends_to(side, distance):
        place = ahead(side, distance)
        inner = (place <= n - 2) if side == 0 else (place >= 1)
        if distance == 1:
            inner = inner | ((z == n - 2) if side == 0 else (z == 1))
        return inner & on_line(place)

    def relays(side):
        return (z == n - 2) if side == 0 else (z == 1)

    causal_line = lax.broadcasted_iota(jnp.int32, (2 * TILE, TILE), 0)
    causal_lane = lax.broadcasted_iota(jnp.int32, (2 * TILE, TILE), 1)
    causal_line = jnp.where(causal_line >= TILE, causal_line - TILE, causal_line)
    causal = (causal_line // steps == causal_lane // steps) & (causal_lane <= causal_line)

    def new_part(c):
        for half in range(2):
            for pair in range(half * (pairs // 2), (half + 1) * (pairs // 2)):
                scores = nt(asked(c, pair), new_keys[...])
                plain = scores[:, :fresh]
                tail = jnp.where(causal, scores[:, fresh:], FAR)
                before = top[c * pairs + pair][:, :1]
                highest = jnp.maximum(
                    jnp.maximum(before, jnp.max(plain, 1, keepdims=True)),
                    jnp.max(tail, 1, keepdims=True),
                )
                weight = jnp.exp2((plain - highest) * factor).astype(bf16)
                tail_weight = jnp.exp2((tail - highest) * factor).astype(bf16)
                weight = jnp.concatenate([weight, tail_weight], 1)
                total = mixed[c * pairs + pair] * jnp.exp2((before - highest) * factor)
                total = total + jnp.dot(weight, new_values[...], preferred_element_type=f32)
                mean = (total[:, :HD] / total[:, HD:]).astype(bf16)
                for k in range(2):
                    column = pl.ds((2 * pair + k) * HD, HD)
                    gathered[z, at(c), column] = mean[k * TILE : (k + 1) * TILE]

            for distance in range(max(1, n - 2), 0, -1):
                for side in (0, 1):

                    @pl.when(sends_to(side, distance))
                    def _():
                        ag_copy(side, distance, c, half).start()

    @pl.loop(0, min(2, chunks))
    def _(c):
        cached_part(c)

    finish_span()

    @pl.loop(2, max(2, chunks))
    def _(c):
        cached_part(c)

    if n > 2:
        for c in range(1, chunks):
            relay_step(c, 1)
    wait_span()
    for c in range(chunks):
        finish_tail(c)
        new_part(c)
        if c == 0:
            for k in range(2, n - 1):
                for other in range(1, chunks):
                    relay_step(other, k)

    w_load.wait()
    wide = min(512, features)

    def add(origin, block, size, first, half):
        place = pl.ds(pl.multiple_of(block * size, size), size)
        extent = width if half is None else half_heads
        begin = 0 if half is None else half * half_heads
        deep = pl.ds(pl.multiple_of(origin * width + begin, extent), extent)

        @pl.loop(0, features // wide)
        def _(column):
            cols = pl.ds(pl.multiple_of(column * wide, wide), wide)
            term = jnp.dot(
                gathered[origin, place, begin : begin + extent],
                w_all[deep, cols],
                preferred_element_type=f32,
            )
            if first:
                acc[place, cols] = term
            else:
                acc[place, cols] += term

    def out_copy(c):
        place = pl.ds(c * group, group)
        return pltpu.make_async_copy(result.at[place], out.at[place], out_sem.at[c])

    tall = min(2 * TILE, number)

    @pl.loop(0, number // tall)
    def _(block):
        add(z, block, tall, True, None)

    def output(c):
        for distance in range(1, n):
            for side in (0, 1):

                @pl.when(on_line(behind(side, distance)))
                def _():
                    for half in range(2):
                        ag_arrival(side, distance, c, half).wait_recv()
                        if distance < n - 1:

                            @pl.when(relays(side))
                            def _():
                                ag_relay(side, distance, c, half).start()

                        add(behind(side, distance), c, TILE, False, half)

        place = pl.ds(c * group, group)

        @pl.loop(0, features // wide)
        def _(column):
            cols = pl.ds(pl.multiple_of(column * wide, wide), wide)
            done = acc[at(c), cols].astype(bf16)
            result[place, :, cols] = done.reshape(group, steps, wide)

        out_copy(c).start()

    @pl.loop(0, chunks - 1)
    def _(c):
        output(c)

    for kind in range(chunks + 1):
        for distance in range(1, n):
            for side in (0, 1):

                @pl.when(direct(kind, side, distance))
                def _():
                    sp_copy(kind, side, distance).wait_send()

    for k in range(1, n_rep):
        nk_copy(new_keys, 0, k, rep).wait_send()
        nk_copy(new_values, 1, k, rep).wait_send()
    for side in (0, 1):

        @pl.when(jnp.logical_not(z == last(side)))
        def _():
            for c in range(1, chunks):
                hop(side, c).wait_send()

        for distance in range(1, max(2, n - 1)):

            @pl.when(sends_to(side, distance))
            def _():
                @pl.loop(0, chunks)
                def _(c):
                    for half in range(2):
                        ag_copy(side, distance, c, half).wait_send()

    output(chunks - 1)
    for side in (0, 1):
        for distance in range(1, n - 1):

            @pl.when(relays(side) & on_line(behind(side, distance)))
            def _():
                @pl.loop(0, chunks)
                def _(c):
                    for half in range(2):
                        ag_relay(side, distance, c, half).wait_send()

    @pl.loop(0, chunks)
    def _(c):
        out_copy(c).wait()


def on_device(
    prompt_owner,
    fork_map,
    page_table,
    prompt_length,
    span_states,
    decode_states,
    decode_queries,
    key_weight,
    value_weight,
    out_weight,
    page_pool,
):
    n_replica = lax.axis_size("replica")
    n_tensor = lax.axis_size("tensor")
    span = span_states.shape[0]
    rows, steps, width = decode_states.shape
    heads_width = decode_queries.shape[2]
    heads_dev = heads_width // HD
    kv_heads = key_weight.shape[1] // HD
    number = rows * steps
    if (
        kv_heads != n_tensor
        or n_tensor < 2
        or n_replica < 2
        or span % TILE
        or number % TILE
        or number % min(2 * TILE, number)
        or TILE % steps
        or heads_dev % 4
        or n_replica > HD
    ):
        return general(
            prompt_owner, fork_map, page_table, prompt_length, span_states, decode_states,
            decode_queries, key_weight, value_weight, out_weight, page_pool,
        )
    features = out_weight.shape[1]
    pages, page_size = page_pool.shape[1], page_pool.shape[2]
    cached = pages * page_size
    fresh = n_replica * span + TILE
    chunks = number // TILE
    two = 2 * HD
    pairs = chunks * heads_dev // 2
    inner = max(1, n_tensor - 2)
    kinds, later = chunks + 1, max(1, chunks - 1)
    bf16, f32 = jnp.bfloat16, jnp.float32
    dma = pltpu.SemaphoreType.DMA
    vmem, smem = pltpu.VMEM, pl.BlockSpec(memory_space=pltpu.SMEM)
    whole = pl.BlockSpec(memory_space=pltpu.VMEM)
    return pl.pallas_call(
        functools.partial(fused, n_tensor, n_replica, steps),
        name="fused",
        out_shape=jax.ShapeDtypeStruct((rows, steps, features), bf16),
        in_specs=[smem] * 3 + [whole] + [pl.BlockSpec(memory_space=pl.ANY)] * 7,
        out_specs=pl.BlockSpec(memory_space=pl.ANY),
        scratch_shapes=[
            vmem(span_states.shape, bf16),
            vmem(decode_states.shape, bf16),
            vmem(decode_queries.shape, bf16),
            vmem((number, heads_width), bf16),
            vmem((width, n_tensor * two), bf16),
            vmem(out_weight.shape, bf16),
            vmem(page_pool.shape[1:], bf16),
            vmem((number, HD), bf16),
            vmem((span + number, HD), f32),
            vmem((span + number, HD), f32),
            vmem((kinds, n_tensor, max(span, TILE), two), bf16),
            vmem((kinds, n_tensor, max(span, TILE), two), f32),
            vmem((kinds, 2, n_tensor - 1, max(span, TILE), two), bf16),
            vmem((2, later, TILE, two), bf16),
            vmem((2, later, TILE, two), bf16),
            vmem((cached, two), bf16),
            vmem((cached, two), bf16),
            vmem((fresh, two), bf16),
            vmem((fresh, two), bf16),
            vmem((pairs, 2 * TILE, two), f32),
            vmem((pairs, 2 * TILE, HD), f32),
            vmem((n_tensor, number, heads_width), bf16),
            vmem((number, features), f32),
            vmem((rows, steps, features), bf16),
            dma((2 * n_tensor + chunks + 4,)),
            dma((kinds, 2, n_tensor - 1)),
            dma((kinds, 2, n_tensor - 1)),
            dma((2, later)),
            dma((2, later)),
            dma((2, n_replica - 1)),
            dma((2, n_replica - 1)),
            dma((2, inner, chunks, 2)),
            dma((2, n_tensor - 1, chunks, 2)),
            dma((2, inner, chunks, 2)),
            dma((chunks,)),
        ],
        compiler_params=pltpu.CompilerParams(
            collective_id=0, has_side_effects=True, vmem_limit_bytes=62 * 1024 * 1024
        ),
    )(
        prompt_owner, prompt_length, page_table, fork_map.reshape(1, rows), span_states,
        decode_states, decode_queries, key_weight, value_weight, out_weight,
        page_pool.reshape(page_pool.shape[1:]),
    )


def solution(mesh):
    in_specs = (
        P("parts"),
        P(("parts", "replica")),
        P("parts"),
        P("parts"),
        P(("parts", "replica"), "tensor"),
        P(("parts", "replica"), None, "tensor"),
        P(("parts", "replica"), None, "tensor"),
        P("tensor", None),
        P("tensor", None),
        P(None, "tensor"),
        P("tensor", "parts", None, None),
    )
    out_specs = P(("parts", "replica"), None, "tensor")
    return jax.shard_map(
        on_device, mesh=mesh, in_specs=in_specs, out_specs=out_specs, check_vma=False
    )
```

```python
import functools
import math

import jax
import jax.numpy as jnp
from jax import lax
from jax.experimental import pallas as pl
from jax.experimental.pallas import tpu as pltpu
from jax.sharding import PartitionSpec as P

HD = 128


rope_base = 1000000.0


def rotary(vectors, places):
    half = vectors.shape[-1] // 2
    freq = rope_base ** (-(2.0 / vectors.shape[-1]) * jnp.arange(half, dtype=jnp.float32))
    angle = places.astype(jnp.float32)[..., None, None] * freq
    cosine = jnp.cos(angle)
    sine = jnp.sin(angle)
    first = vectors[..., :half]
    second = vectors[..., half:]
    return jnp.concatenate([first * cosine - second * sine, second * cosine + first * sine], -1)


def rotate_round(summed, places, kv_heads):
    number = summed.shape[0]
    turned = rotary(summed[:, : kv_heads * HD].reshape(number, kv_heads, HD), places)
    turned = turned.astype(jnp.bfloat16).reshape(number, kv_heads * HD)
    return jnp.concatenate([turned, summed[:, kv_heads * HD :].astype(jnp.bfloat16)], 1)


def own_pair(packed, head_group, kv_heads):
    key_part = lax.dynamic_slice_in_dim(packed, head_group * HD, HD, 1)
    value_part = lax.dynamic_slice_in_dim(packed, (kv_heads + head_group) * HD, HD, 1)
    return jnp.concatenate([key_part, value_part], 1)


def general(
    prompt_owner,
    fork_map,
    page_table,
    prompt_length,
    span_states,
    decode_states,
    decode_queries,
    key_weight,
    value_weight,
    out_weight,
    page_pool,
):
    replica = lax.axis_index("replica")
    device_rank = lax.axis_index("tensor")
    n_replica = lax.axis_size("replica")
    n_tensor = lax.axis_size("tensor")
    span = span_states.shape[0]
    rows, steps, width = decode_states.shape
    heads_dev = decode_queries.shape[2] // HD
    kv_heads = key_weight.shape[1] // HD
    sharing = n_tensor // kv_heads
    prompts = jnp.arange(n_replica, dtype=jnp.int32)
    own_prompt = jnp.sum(jnp.where(prompts == replica, prompt_owner, 0))
    own_length = jnp.sum(jnp.where(prompts == own_prompt, prompt_length, 0))
    row_hits = fork_map[:, None] == prompts[None, :]
    row_length = jnp.sum(jnp.where(row_hits, prompt_length[None, :], 0), 1)
    positions = jnp.concatenate(
        [
            own_length + jnp.arange(span, dtype=jnp.int32),
            (row_length[:, None] + span + jnp.arange(steps, dtype=jnp.int32)[None, :]).reshape(-1),
        ]
    )
    tokens = jnp.concatenate([span_states, decode_states.reshape(rows * steps, width)], 0)
    projected = jnp.dot(
        tokens, jnp.concatenate([key_weight, value_weight], 1), preferred_element_type=jnp.float32
    )
    share = lax.psum_scatter(projected, "tensor", scatter_dimension=0, tiled=True)
    number = share.shape[0]
    start = device_rank * number
    places = lax.dynamic_slice_in_dim(positions, start, number)
    turned = rotate_round(share, places, kv_heads)
    groups = jnp.stack(
        [own_pair(turned, group_index, kv_heads) for group_index in range(kv_heads)], 0
    )
    outgoing = jnp.repeat(groups, sharing, axis=0)
    paired = lax.all_to_all(outgoing, "tensor", split_axis=0, concat_axis=1, tiled=True).reshape(
        -1, 2 * HD
    )
    arrived = lax.all_gather(paired[:span], "replica", axis=0, tiled=True)
    tail_pair = paired[span:].reshape(rows, steps, 2 * HD)
    pool_pages = page_table.shape[0]
    cpages = pool_pages // n_replica
    page_size = page_pool.shape[2]
    entries = jnp.arange(pool_pages, dtype=jnp.int32)
    page_hits = page_table[None, :] == entries[:, None]
    page_prompt = jnp.sum(jnp.where(page_hits, entries[None, :] // cpages, 0), 1)
    page_slot = jnp.sum(jnp.where(page_hits, entries[None, :] % cpages, 0), 1)
    page_length = jnp.sum(
        jnp.where(page_prompt[:, None] == prompts[None, :], prompt_length[None, :], 0), 1
    )
    visible = (
        page_slot[:, None] * page_size + jnp.arange(page_size, dtype=jnp.int32)[None, :]
        < page_length[:, None]
    )
    pool_prompt = jnp.where(visible, page_prompt[:, None], -1).reshape(-1)
    key_prompt = jnp.concatenate([pool_prompt, jnp.repeat(prompt_owner, span)])
    key_table = jnp.concatenate([page_pool.reshape(-1, 2 * HD), arrived], 0)
    cached_keys = key_table[:, :HD]
    cached_values = key_table[:, HD:]
    scale = 1.0 / math.sqrt(HD)
    causal = jnp.arange(steps)[None, :] <= jnp.arange(steps)[:, None]
    per_block = max(1, min(rows, 512 // (steps * heads_dev)))
    blocks = rows // per_block
    queries = decode_queries.reshape(blocks, per_block, steps, heads_dev, HD)

    def attend(items):
        query, prompt, own_tail = items
        flat = query.reshape(-1, HD)
        scores = (
            lax.dot_general(
                flat, cached_keys, (((1,), (1,)), ((), ())), preferred_element_type=jnp.float32
            )
            * scale
        )
        scores = scores.reshape(per_block, steps, heads_dev, -1)
        allowed = (key_prompt[None, :] == prompt[:, None])[:, None, None, :]
        scores = jnp.where(allowed, scores, -jnp.inf)
        tail_scores = (
            jnp.einsum(
                "rshd,rtd->rsht", query, own_tail[..., :HD], preferred_element_type=jnp.float32
            )
            * scale
        )
        tail_scores = jnp.where(causal[None, :, None, :], tail_scores, -jnp.inf)
        highest = jnp.maximum(jnp.max(scores, -1), jnp.max(tail_scores, -1))
        weight = jnp.exp(scores - highest[..., None])
        tail_weight = jnp.exp(tail_scores - highest[..., None])
        total = jnp.sum(weight, -1) + jnp.sum(tail_weight, -1)
        rounded = weight.astype(jnp.bfloat16).reshape(-1, weight.shape[-1])
        mixed = jnp.dot(rounded, cached_values, preferred_element_type=jnp.float32).reshape(
            per_block, steps, heads_dev, HD
        )
        mixed = mixed + jnp.einsum(
            "rsht,rtd->rshd",
            tail_weight.astype(jnp.bfloat16),
            own_tail[..., HD:],
            preferred_element_type=jnp.float32,
        )
        return (mixed / total[..., None]).astype(jnp.bfloat16)

    attended = lax.map(
        attend,
        (
            queries,
            fork_map.reshape(blocks, per_block),
            tail_pair.reshape(blocks, per_block, steps, 2 * HD),
        ),
    )
    head_rows = attended.reshape(rows * steps, heads_dev * HD)
    decoded = jnp.dot(
        lax.all_gather(head_rows, "tensor", axis=1, tiled=True),
        out_weight,
        preferred_element_type=jnp.float32,
    )
    return decoded.astype(jnp.bfloat16).reshape(rows, steps, width)


MESH_ID = pl.DeviceIdType.MESH
TILE = 128
FAR = -(2.0**100)


def nt(left, right):
    return lax.dot_general(
        left, right, (((1,), (1,)), ((), ())), preferred_element_type=jnp.float32
    )


def fused(
    n, n_rep, steps, owner_s, length_s, table_s, fork, span_hbm, dec_hbm, query_hbm, wk_hbm,
    wv_hbm, w_hbm, pool_hbm, out,
    span_tok, dec_tok, query_in, query, w_kv, w_all, pool, hot, cosine, sine,
    part, own, landed, hop_out, hop_in, keys, values, new_keys, new_values,
    mixed, top, gathered, acc, result,
    in_sem, sp_send, sp_recv, rs_send, rs_recv, nk_send, nk_recv, ag_send, ag_recv, out_sem,
):
    z = lax.axis_index("tensor")
    rep = lax.axis_index("replica")
    bf16, f32 = jnp.bfloat16, jnp.float32
    span, depth = span_tok.shape
    rows = dec_tok.shape[0]
    number = rows * steps
    chunks = number // TILE
    group = TILE // steps
    width = query.shape[1]
    heads = width // HD
    pairs = heads // 2
    pages, page_size = pool.shape[0], pool.shape[1]
    cpages = pages // n_rep
    features = w_all.shape[1]
    two = 2 * HD
    factor = math.log2(math.e) / math.sqrt(HD)

    def at(block):
        if isinstance(block, int):
            return pl.ds(block * TILE, TILE)
        return pl.ds(pl.multiple_of(block * TILE, TILE), TILE)

    def load(src, dst, slot):
        return pltpu.make_async_copy(src, dst, in_sem.at[slot])

    loads = [load(span_hbm, span_tok, 0)]
    for d in range(n):
        column = pl.ds(d * HD, HD)
        loads.append(load(wk_hbm.at[:, column], w_kv.at[:, pl.ds(d * two, HD)], 1 + 2 * d))
        loads.append(load(wv_hbm.at[:, column], w_kv.at[:, pl.ds(d * two + HD, HD)], 2 + 2 * d))
    first_dec = len(loads)
    for c in range(chunks):
        piece = pl.ds(c * group, group)
        loads.append(load(dec_hbm.at[piece], dec_tok.at[piece], first_dec + c))
    pool_load = load(pool_hbm, pool, first_dec + chunks)
    query_load = load(query_hbm, query_in, first_dec + chunks + 1)
    w_load = load(w_hbm, w_all, first_dec + chunks + 2)
    for item in loads:
        item.start()
    pool_load.start()
    query_load.start()

    barrier = pltpu.get_barrier_semaphore()
    for k in range(1, n):
        pl.semaphore_signal(
            barrier, inc=1, device_id={"tensor": lax.rem(z + k, n)}, device_id_type=MESH_ID
        )
    for k in range(1, n_rep):
        pl.semaphore_signal(
            barrier, inc=1, device_id={"replica": lax.rem(rep + k, n_rep)}, device_id_type=MESH_ID
        )

    def turns(places, block):
        lane = lax.broadcasted_iota(jnp.int32, (TILE, HD), 1)
        half = HD // 2
        low = lane < half
        power = jnp.where(low, lane, lane - half).astype(f32) * (-(2.0 / HD) * math.log(rope_base))
        angle = places * jnp.exp(power)
        cosine[at(block), :] = jnp.cos(angle)
        turned = jnp.sin(angle)
        sine[at(block), :] = jnp.where(low, -turned, turned)

    own_length = length_s[owner_s[rep]]
    for block in range(span // TILE):
        line = lax.broadcasted_iota(jnp.int32, (TILE, HD), 0)
        turns((line + (own_length + block * TILE)).astype(f32), block)

    for item in loads[:first_dec]:
        item.wait()
    pl.semaphore_wait(barrier, n + n_rep - 2)
    def keep(kind, block, tokens):
        term = jnp.dot(tokens, w_kv[...], preferred_element_type=f32)
        for d in range(n):
            part[kind, d, at(block), :] = term[:, d * two : (d + 1) * two].astype(bf16)
            own[kind, d, at(block), :] = term[:, d * two : (d + 1) * two]

    for block in range(span // TILE):
        keep(0, block, span_tok[at(block), :])

    def ahead(side, distance):
        return z + distance - 2 * side * distance

    def behind(side, distance):
        return ahead(1 - side, distance)

    def on_line(place):
        return (place >= 0) & (place < n)

    def sized(kind):
        return pl.ds(0, span if kind == 0 else TILE)

    def sp_copy(kind, side, distance):
        target = ahead(side, distance)
        return pltpu.make_async_remote_copy(
            src_ref=part.at[kind, target, sized(kind)],
            dst_ref=landed.at[kind, side, distance - 1, sized(kind)],
            send_sem=sp_send.at[kind, side, distance - 1],
            recv_sem=sp_recv.at[kind, side, distance - 1],
            device_id={"tensor": target},
            device_id_type=MESH_ID,
        )

    def sp_arrival(kind, side, distance):
        return pltpu.make_async_remote_copy(
            src_ref=part.at[kind, 0, sized(kind)],
            dst_ref=landed.at[kind, side, distance - 1, sized(kind)],
            send_sem=sp_send.at[kind, side, distance - 1],
            recv_sem=sp_recv.at[kind, side, distance - 1],
            device_id={"tensor": lax.rem(z + 1, n)},
            device_id_type=MESH_ID,
        )

    def inner(place):
        return (place >= 1) & (place <= n - 2)

    def direct(kind, side, distance):
        place = ahead(side, distance)
        return on_line(place) if kind < 2 else inner(place)

    def scatter(kind, ends):
        for distance in range(n - 1, 0, -1):
            for side in (0, 1):
                place = ahead(side, distance)
                target = on_line(place) & jnp.logical_not(inner(place)) if ends else inner(place)

                @pl.when(target)
                def _():
                    sp_copy(kind, side, distance).start()

    def collect(kind):
        for side in (0, 1):
            for distance in range(1, n):

                here = on_line(behind(side, distance))

                @pl.when(here if kind < 2 else here & inner(z))
                def _():
                    sp_arrival(kind, side, distance).wait_recv()
                    own[kind, z, sized(kind)] = own[kind, z, sized(kind)] + landed[
                        kind, side, distance - 1, sized(kind)
                    ].astype(f32)

    def decode_tokens(c):
        loads[first_dec + c].wait()
        return dec_tok[pl.ds(c * group, group)].reshape(TILE, depth)

    def hop(side, kind):
        return pltpu.make_async_remote_copy(
            src_ref=hop_out.at[side, kind, sized(kind)],
            dst_ref=hop_in.at[side, kind, sized(kind)],
            send_sem=rs_send.at[side, kind],
            recv_sem=rs_recv.at[side, kind],
            device_id={"tensor": jnp.clip(ahead(side, 1), 0, n - 1)},
            device_id_type=MESH_ID,
        )

    def last(side):
        return n - 1 if side == 0 else 0

    def hop_first(kind):
        for side in (0, 1):

            @pl.when(z == last(1 - side))
            def _():
                hop_out[side, kind, sized(kind)] = part[kind, last(side), sized(kind)]
                hop(side, kind).start()

    def relay_step(kind, k):
        for side, node in ((0, k), (1, n - 1 - k)):

            @pl.when(z == node)
            def _():
                hop(side, kind).wait_recv()
                total = own[kind, last(side), sized(kind)]
                total = total + hop_in[side, kind, sized(kind)].astype(f32)
                hop_out[side, kind, sized(kind)] = total.astype(bf16)
                hop(side, kind).start()

    def arrive_end(kind):
        for side in (0, 1):

            @pl.when(z == last(side))
            def _():
                hop(side, kind).wait_recv()
                own[kind, z, sized(kind)] = own[kind, z, sized(kind)] + hop_in[
                    side, kind, sized(kind)
                ].astype(f32)

    scatter(0, False)
    keep(1, 0, decode_tokens(0))
    scatter(1, False)
    scatter(0, True)
    scatter(1, True)
    w_load.start()
    for c in range(1, chunks):
        keep(c + 1, 0, decode_tokens(c))
        scatter(c + 1, False)
    for c in range(1, chunks):
        hop_first(c + 1)

    def rotate(total, block):
        key = total[:, :HD]
        key = key * cosine[at(block), :] + pltpu.roll(key, HD // 2, 1) * sine[at(block), :]
        return key.astype(bf16), total[:, HD:].astype(bf16)


    prompt_of = lax.broadcasted_iota(jnp.int32, (HD, rows), 0)
    chosen = (prompt_of == fork[...]).astype(f32).astype(bf16)
    lanes = lax.broadcasted_iota(jnp.int32, (TILE, HD), 1)
    lines = lax.broadcasted_iota(jnp.int32, (TILE, HD), 0)
    lengths = jnp.zeros((TILE, HD), f32)
    for p in range(n_rep):
        lengths = jnp.where(lanes == p, length_s[p].astype(f32), lengths)
    for c in range(chunks):
        line = lax.broadcasted_iota(jnp.int32, (TILE, rows), 0)
        lane = lax.broadcasted_iota(jnp.int32, (TILE, rows), 1)
        belongs = (line // steps + c * group == lane).astype(f32).astype(bf16)
        one_hot = nt(belongs, chosen)
        hot[at(c), :] = one_hot.astype(bf16)
        length = jnp.sum(one_hot * lengths, 1, keepdims=True)
        turns(length + (lines % steps + span).astype(f32), c + span // TILE)

    pool_load.wait()
    for j in range(pages):
        p = j // cpages
        start = (j % cpages) * page_size
        place = pl.ds(j * page_size, page_size)
        page = pool[table_s[j]]
        line = lax.broadcasted_iota(jnp.int32, (page_size, HD), 0)
        lane = lax.broadcasted_iota(jnp.int32, (page_size, HD), 1)
        seen = (lane == p) & (line + start < length_s[p])
        keys[place, :HD] = page[:, :HD]
        keys[place, HD:] = jnp.where((lane >= n_rep) | seen, 0.0, FAR).astype(bf16)
        values[place, :HD] = page[:, HD:]
        values[place, HD:] = jnp.ones((page_size, HD), bf16)

    fresh = n_rep * span
    for r in range(n_rep):
        lane = lax.broadcasted_iota(jnp.int32, (span, HD), 1)
        place = pl.ds(r * span, span)
        near = (lane >= n_rep) | (lane == owner_s[r])
        new_keys[place, HD:] = jnp.where(near, 0.0, FAR).astype(bf16)
    new_keys[pl.ds(fresh, TILE), HD:] = jnp.zeros((TILE, HD), bf16)
    new_values[:, HD:] = jnp.ones((new_values.shape[0], HD), bf16)

    query_load.wait()
    for c in range(chunks):
        query[at(c), :] = query_in[pl.ds(c * group, group)].reshape(TILE, width)

    def asked(c, pair):
        asks = []
        for k in range(2):
            column = pl.ds((2 * pair + k) * HD, HD)
            asks.append(jnp.concatenate([query[at(c), column], hot[at(c), :]], 1))
        return jnp.concatenate(asks, 0)

    def cached_part(c):
        for pair in range(pairs):
            scores = nt(asked(c, pair), keys[...])
            highest = jnp.max(scores, 1, keepdims=True)
            weight = jnp.exp2((scores - highest) * factor).astype(bf16)
            mixed[c * pairs + pair] = jnp.dot(weight, values[...], preferred_element_type=f32)
            top[c * pairs + pair] = jnp.broadcast_to(highest, (2 * TILE, HD))

    def nk_copy(array, kind, k, whose):
        place = pl.ds(pl.multiple_of(whose * span, span), span)
        return pltpu.make_async_remote_copy(
            src_ref=array.at[place, pl.ds(0, HD)],
            dst_ref=array.at[place, pl.ds(0, HD)],
            send_sem=nk_send.at[kind, k - 1],
            recv_sem=nk_recv.at[kind, k - 1],
            device_id={"replica": lax.rem(rep + k, n_rep)},
            device_id_type=MESH_ID,
        )

    def finish_span():
        collect(0)
        for block in range(span // TILE):
            key, value = rotate(own[0, z, at(block), :], block)
            place = pl.ds(pl.multiple_of(rep * span + block * TILE, TILE), TILE)
            new_keys[place, :HD] = key
            new_values[place, :HD] = value
        for k in range(1, n_rep):
            nk_copy(new_keys, 0, k, rep).start()
            nk_copy(new_values, 1, k, rep).start()

    def wait_span():
        for k in range(1, n_rep):
            whose = lax.rem(rep - k + n_rep, n_rep)
            nk_copy(new_keys, 0, k, whose).wait_recv()
            nk_copy(new_values, 1, k, whose).wait_recv()

    def place_tail(total, c):
        key, value = rotate(total, c + span // TILE)
        new_keys[pl.ds(fresh, TILE), :HD] = key
        new_values[pl.ds(fresh, TILE), :HD] = value

    def finish_tail(c):
        collect(c + 1)
        if c > 0:
            arrive_end(c + 1)
        place_tail(own[c + 1, z, sized(c + 1)], c)

    half_heads = width // 2

    def block_of(origin, c, half):
        column = pl.ds(half * half_heads, half_heads)
        return gathered.at[origin, at(c), column]

    def ag_copy(side, distance, c, half):
        origin = behind(side, distance)
        return pltpu.make_async_remote_copy(
            src_ref=block_of(origin, c, half),
            dst_ref=block_of(origin, c, half),
            send_sem=ag_send.at[side, distance, c, half],
            recv_sem=ag_recv.at[side, distance, c, half],
            device_id={"tensor": jnp.clip(ahead(side, 1), 0, n - 1)},
            device_id_type=MESH_ID,
        )

    def ag_arrival(side, distance, c, half):
        origin = behind(side, distance)
        return pltpu.make_async_remote_copy(
            src_ref=block_of(origin, c, half),
            dst_ref=block_of(origin, c, half),
            send_sem=ag_send.at[side, 0, c, half],
            recv_sem=ag_recv.at[side, distance - 1, c, half],
            device_id={"tensor": jnp.clip(ahead(side, 1), 0, n - 1)},
            device_id_type=MESH_ID,
        )

    busy = jnp.where(z >= n // 2, 0, 1)

    def send_own(side, c, half):
        @pl.when(on_line(ahead(side, 1)))
        def _():
            ag_copy(side, 0, c, half).start()

    causal_line = lax.broadcasted_iota(jnp.int32, (2 * TILE, TILE), 0)
    causal_lane = lax.broadcasted_iota(jnp.int32, (2 * TILE, TILE), 1)
    causal_line = jnp.where(causal_line >= TILE, causal_line - TILE, causal_line)
    causal = (causal_line // steps == causal_lane // steps) & (causal_lane <= causal_line)

    def new_part(c):
        for half in range(2):
            for pair in range(half * (pairs // 2), (half + 1) * (pairs // 2)):
                scores = nt(asked(c, pair), new_keys[...])
                plain = scores[:, :fresh]
                tail = jnp.where(causal, scores[:, fresh:], FAR)
                before = top[c * pairs + pair][:, :1]
                highest = jnp.maximum(
                    jnp.maximum(before, jnp.max(plain, 1, keepdims=True)),
                    jnp.max(tail, 1, keepdims=True),
                )
                weight = jnp.exp2((plain - highest) * factor).astype(bf16)
                tail_weight = jnp.exp2((tail - highest) * factor).astype(bf16)
                weight = jnp.concatenate([weight, tail_weight], 1)
                total = mixed[c * pairs + pair] * jnp.exp2((before - highest) * factor)
                total = total + jnp.dot(weight, new_values[...], preferred_element_type=f32)
                mean = (total[:, :HD] / total[:, HD:]).astype(bf16)
                for k in range(2):
                    column = pl.ds((2 * pair + k) * HD, HD)
                    gathered[z, at(c), column] = mean[k * TILE : (k + 1) * TILE]

            send_own(busy, c, half)
            if c < 2:
                send_own(1 - busy, c, half)

    def ask(low, high):
        @pl.loop(low, max(low, min(high, chunks)))
        def _(c):
            cached_part(c)

    ask(0, 1)
    finish_span()
    ask(1, 3)
    wait_span()
    finish_tail(0)
    new_part(0)
    ask(3, chunks)

    def relay_all(k):
        for kind in range(2, chunks + 1):
            relay_step(kind, k)

    for c in range(1, chunks):
        finish_tail(c)
        new_part(c)
    for k in range(1, n - 1):
        relay_all(k)
        if k == 1:
            for c in range(2, chunks):
                for half in range(2):
                    send_own(1 - busy, c, half)
    if n == 2:
        for c in range(2, chunks):
            for half in range(2):
                send_own(1 - busy, c, half)

    w_load.wait()
    wide = min(512, features)

    def add(origin, block, size, first, half):
        place = pl.ds(pl.multiple_of(block * size, size), size)
        extent = width if half is None else half_heads
        begin = 0 if half is None else half * half_heads
        deep = pl.ds(pl.multiple_of(origin * width + begin, extent), extent)

        @pl.loop(0, features // wide)
        def _(column):
            cols = pl.ds(pl.multiple_of(column * wide, wide), wide)
            term = jnp.dot(
                gathered[origin, place, begin : begin + extent],
                w_all[deep, cols],
                preferred_element_type=f32,
            )
            if first:
                acc[place, cols] = term
            else:
                acc[place, cols] += term

    def out_copy(c):
        place = pl.ds(c * group, group)
        return pltpu.make_async_copy(result.at[place], out.at[place], out_sem.at[c])

    tall = min(2 * TILE, number)

    @pl.loop(0, number // tall)
    def _(block):
        add(z, block, tall, True, None)

    def output(c):
        place = pl.ds(c * group, group)

        @pl.loop(0, features // wide)
        def _(column):
            cols = pl.ds(pl.multiple_of(column * wide, wide), wide)
            done = acc[at(c), cols].astype(bf16)
            result[place, :, cols] = done.reshape(group, steps, wide)

        out_copy(c).start()

    def arrivals(distance, side, c):
        @pl.when(on_line(behind(side, distance)))
        def _():
            for half in range(2):
                ag_arrival(side, distance, c, half).wait_recv()
                if distance < n - 1:

                    @pl.when(on_line(ahead(side, 1)))
                    def _():
                        ag_copy(side, distance, c, half).start()

                add(behind(side, distance), c, TILE, False, half)

    for distance in range(1, n - 1):
        for side in (busy, 1 - busy):

            @pl.loop(0, chunks)
            def _(c):
                arrivals(distance, side, c)

    for kind in range(chunks + 1):
        for distance in range(1, n):
            for side in (0, 1):

                @pl.when(direct(kind, side, distance))
                def _():
                    sp_copy(kind, side, distance).wait_send()

    for k in range(1, n_rep):
        nk_copy(new_keys, 0, k, rep).wait_send()
        nk_copy(new_values, 1, k, rep).wait_send()
    for side in (0, 1):

        @pl.when(jnp.logical_not(z == last(side)))
        def _():
            for kind in range(2, chunks + 1):
                hop(side, kind).wait_send()

            @pl.loop(0, chunks)
            def _(c):
                for half in range(2):
                    ag_copy(side, 0, c, half).wait_send()

        for distance in range(1, n - 1):

            @pl.when(on_line(ahead(side, 1)) & on_line(behind(side, distance)))
            def _():
                @pl.loop(0, chunks)
                def _(c):
                    for half in range(2):
                        ag_copy(side, distance, c, half).wait_send()

    @pl.loop(0, chunks)
    def _(c):
        arrivals(n - 1, busy, c)
        output(c)

    @pl.loop(0, chunks)
    def _(c):
        out_copy(c).wait()


def on_device(
    prompt_owner,
    fork_map,
    page_table,
    prompt_length,
    span_states,
    decode_states,
    decode_queries,
    key_weight,
    value_weight,
    out_weight,
    page_pool,
):
    n_replica = lax.axis_size("replica")
    n_tensor = lax.axis_size("tensor")
    span = span_states.shape[0]
    rows, steps, width = decode_states.shape
    heads_width = decode_queries.shape[2]
    heads_dev = heads_width // HD
    kv_heads = key_weight.shape[1] // HD
    number = rows * steps
    if (
        kv_heads != n_tensor
        or n_tensor < 2
        or n_replica < 2
        or span % TILE
        or number % TILE
        or number % min(2 * TILE, number)
        or TILE % steps
        or heads_dev % 4
        or n_replica > HD
    ):
        return general(
            prompt_owner, fork_map, page_table, prompt_length, span_states, decode_states,
            decode_queries, key_weight, value_weight, out_weight, page_pool,
        )
    features = out_weight.shape[1]
    pages, page_size = page_pool.shape[1], page_pool.shape[2]
    cached = pages * page_size
    fresh = n_replica * span + TILE
    chunks = number // TILE
    two = 2 * HD
    pairs = chunks * heads_dev // 2
    kinds = chunks + 1
    bf16, f32 = jnp.bfloat16, jnp.float32
    dma = pltpu.SemaphoreType.DMA
    vmem, smem = pltpu.VMEM, pl.BlockSpec(memory_space=pltpu.SMEM)
    whole = pl.BlockSpec(memory_space=pltpu.VMEM)
    return pl.pallas_call(
        functools.partial(fused, n_tensor, n_replica, steps),
        name="fused",
        out_shape=jax.ShapeDtypeStruct((rows, steps, features), bf16),
        in_specs=[smem] * 3 + [whole] + [pl.BlockSpec(memory_space=pl.ANY)] * 7,
        out_specs=pl.BlockSpec(memory_space=pl.ANY),
        scratch_shapes=[
            vmem(span_states.shape, bf16),
            vmem(decode_states.shape, bf16),
            vmem(decode_queries.shape, bf16),
            vmem((number, heads_width), bf16),
            vmem((width, n_tensor * two), bf16),
            vmem(out_weight.shape, bf16),
            vmem(page_pool.shape[1:], bf16),
            vmem((number, HD), bf16),
            vmem((span + number, HD), f32),
            vmem((span + number, HD), f32),
            vmem((kinds, n_tensor, max(span, TILE), two), bf16),
            vmem((kinds, n_tensor, max(span, TILE), two), f32),
            vmem((kinds, 2, n_tensor - 1, max(span, TILE), two), bf16),
            vmem((2, kinds, max(span, TILE), two), bf16),
            vmem((2, kinds, max(span, TILE), two), bf16),
            vmem((cached, two), bf16),
            vmem((cached, two), bf16),
            vmem((fresh, two), bf16),
            vmem((fresh, two), bf16),
            vmem((pairs, 2 * TILE, two), f32),
            vmem((pairs, 2 * TILE, HD), f32),
            vmem((n_tensor, number, heads_width), bf16),
            vmem((number, features), f32),
            vmem((rows, steps, features), bf16),
            dma((2 * n_tensor + chunks + 4,)),
            dma((kinds, 2, n_tensor - 1)),
            dma((kinds, 2, n_tensor - 1)),
            dma((2, kinds)),
            dma((2, kinds)),
            dma((2, n_replica - 1)),
            dma((2, n_replica - 1)),
            dma((2, n_tensor - 1, chunks, 2)),
            dma((2, n_tensor - 1, chunks, 2)),
            dma((chunks,)),
        ],
        compiler_params=pltpu.CompilerParams(
            collective_id=0, has_side_effects=True, vmem_limit_bytes=62 * 1024 * 1024
        ),
    )(
        prompt_owner, prompt_length, page_table, fork_map.reshape(1, rows), span_states,
        decode_states, decode_queries, key_weight, value_weight, out_weight,
        page_pool.reshape(page_pool.shape[1:]),
    )


def solution(mesh):
    in_specs = (
        P("parts"),
        P(("parts", "replica")),
        P("parts"),
        P("parts"),
        P(("parts", "replica"), "tensor"),
        P(("parts", "replica"), None, "tensor"),
        P(("parts", "replica"), None, "tensor"),
        P("tensor", None),
        P("tensor", None),
        P(None, "tensor"),
        P("tensor", "parts", None, None),
    )
    out_specs = P(("parts", "replica"), None, "tensor")
    return jax.shard_map(
        on_device, mesh=mesh, in_specs=in_specs, out_specs=out_specs, check_vma=False
    )
```
